32 devices in a mesh: width: 8 (over z, core), lat: 4 (over y, x).
Axes of the slice: x: 2, y: 2, z: 4, core: 2. Of those that a mesh axis runs over, the one named last changes fastest.
Arguments:
- residuals: bfloat16 [384, 16384], P(None, 'width'), may hold values from -6 to 6
- encoder: bfloat16 [16384, 4096], P('width', 'lat'), may hold values from -0.046875 to 0.046875
- enc_bias: float32 [4096], P('lat'), may hold values from -3 to 3
- decoder: bfloat16 [4096, 16384], P('lat', 'width'), may hold values from -0.046875 to 0.046875
- dec_bias: float32 [16384], P('width'), may hold values from -3 to 3
Outputs:
- enc_grad: bfloat16 [16384, 4096], P('width', 'lat')
- new_decoder: bfloat16 [4096, 16384], P('lat', 'width')
The draws below stay inside these ranges and needn't reach their ends.
All inputs are finite; a program needn't handle non-finite values.
Results may differ from the reference program's by a relative error of at most 0.011.
Values may be sent and summed in bfloat16 or wider, within the bound.
A program may use at most 64 MiB of HBM per device.

```python
import jax
import jax.numpy as jnp
from jax import lax

D = 16384
TOK = 384
LATENTS = 4096
N_LAT = 4


def level_of(rng, shape, shards, least, top_value):
    loudness, own = 1.0, jax.random.fold_in(rng, 6)
    for position, blocks in shards:
        draws = jnp.exp(jax.random.uniform(jax.random.fold_in(own, position), (blocks,), jnp.float32, least / len(shards), top_value / len(shards)))
        loudness = loudness * jnp.repeat(draws, shape[position] // blocks).reshape([-1 if axis == position else 1 for axis in range(len(shape))])
    return loudness


def scatter_about(rng, dims, scale, most, cuts=(), held_as=jnp.bfloat16):
    result = jax.random.normal(rng, dims, jnp.float32) * scale
    if len(cuts) > 0:
        result = level_of(rng, dims, cuts, -0.22, 0.18) * result
    return jnp.clip(result, min=-most, max=most).astype(held_as)


def setup_inputs(seed: int = 0) -> dict:
    key_list = jax.random.split(jax.random.key(seed), 6)
    residuals = scatter_about(key_list[0], (TOK, D), 1.0, 6.0, ((1, 8),))
    encoder = scatter_about(key_list[1], (D, LATENTS), D ** -0.5, 0.046875, ((0, 8), (1, 4)))
    enc_bias = scatter_about(key_list[2], (LATENTS,), 0.5, 3.0, ((0, 4),), jnp.float32)
    decoder = scatter_about(key_list[3], (LATENTS, D), D ** -0.5, 0.046875, ((0, 4), (1, 8)))
    dec_bias = scatter_about(key_list[4], (D,), 0.5, 3.0, ((0, 8),), jnp.float32)
    return dict(residuals=residuals, encoder=encoder, enc_bias=enc_bias, decoder=decoder, dec_bias=dec_bias)


EPS = 1e-06
STEP = 0.0003
PENALTY = 0.5

def reference(residuals, encoder, enc_bias, decoder, dec_bias):
    pre = jnp.dot(residuals, encoder, preferred_element_type=jnp.float32) + enc_bias
    acts = jnp.maximum(pre, 0.0).astype(jnp.bfloat16)
    recon = jnp.dot(acts, decoder, preferred_element_type=jnp.float32)
    error = (recon + dec_bias - residuals.astype(jnp.float32)).astype(jnp.bfloat16)
    dacts = lax.dot_general(error, decoder, (((1,), (1,)), ((), ())), preferred_element_type=jnp.float32) + PENALTY
    dpre = jnp.where(pre > 0.0, dacts, 0.0).astype(jnp.bfloat16)
    enc_grad = lax.dot_general(residuals, dpre, (((0,), (0,)), ((), ())), preferred_element_type=jnp.float32).astype(jnp.bfloat16)
    blocks = N_LAT
    width = acts.shape[1] // blocks
    act_blocks = acts.reshape(acts.shape[0], blocks, width).transpose(1, 0, 2)
    dec_blocks = decoder.reshape(blocks, width, decoder.shape[1])

    def renorm(pair):
        act_blk, dec_blk = pair
        grad = lax.dot_general(act_blk, error, (((0,), (0,)), ((), ())), preferred_element_type=jnp.float32)
        weight = dec_blk.astype(jnp.float32)
        ww = lax.optimization_barrier(jnp.sum(weight * weight, axis=1, keepdims=True))
        gw = lax.optimization_barrier(jnp.sum(grad * weight, axis=1, keepdims=True))
        coef = gw / (ww + EPS)
        moved = weight - STEP * (grad - coef * weight)
        squared = lax.optimization_barrier(jnp.sum(moved * moved, axis=1, keepdims=True))
        return (moved / jnp.sqrt(squared + EPS)).astype(jnp.bfloat16)
    new_decoder = lax.map(renorm, (act_blocks, dec_blocks)).reshape(decoder.shape)
    return (enc_grad, new_decoder)
```

```python
import functools

import jax
import jax.numpy as jnp
from jax import lax
from jax.experimental import pallas as pl
from jax.experimental.pallas import tpu as pltpu
from jax.sharding import PartitionSpec as P

EPS = 1e-06
STEP = 0.0003
PENALTY = 0.5
MESH = pl.DeviceIdType.MESH
F32, BF16 = jnp.float32, jnp.bfloat16
NT = (((1,), (1,)), ((), ()))


def step_kernel(
    Z, NL, NK, NN,
    res_h, enc_h, bias_h, dec_h, dbias_h,
    nd_v, dp, rt_v,
    res_v, enc_v, dec_v, bias, dbias, stA, rxA, sA, rA, preS, acts, actsT,
    rf, sB, rB, err, dacc, sD, rxD, sS, rD, grad, sacc, stv, rst, ss, rs2, st,
    in_sem,
    a1s, a1r, a2s, a2r, a3s, a3r, a4s, a4r,
    bs, br, cs, cr,
    d1s, d1r, d2s, d2r, d3s, d3r, d4s, d4r,
    e1s, e1r, e2s, e2r,
):
    T, DW = res_v.shape
    H = acts.shape[0]
    TH = T // H
    TB, KC = acts.shape[-2:]
    KB = 2 * KC
    TL, NB = err.shape[-2:]
    w = lax.axis_index("width")
    l = lax.axis_index("lat")
    z, c = w // 2, w % 2
    pc = 1 - c
    partner = (z * 2 + pc, l)

    def zdev(o):
        return ((z + o) % Z) * 2 + c, l

    def lat_to(o):
        return ((l // 2 + o // 2) % (NL // 2)) * 2 + (l % 2 + o % 2) % 2

    def lat_from(o):
        return ((l // 2 + NL // 2 - o // 2) % (NL // 2)) * 2 + (l % 2 + o % 2) % 2

    def rc(src, dst, ssem, rsem, dev):
        return pltpu.make_async_remote_copy(
            src_ref=src, dst_ref=dst, send_sem=ssem, recv_sem=rsem,
            device_id=dev, device_id_type=MESH,
        )

    def loop(n, f):
        lax.fori_loop(0, n, lambda i, _: (f(i), 0)[1], 0)

    c_res = pltpu.make_async_copy(res_h, res_v, in_sem.at[0])
    c_res.start()

    def enc_copy(k):
        return pltpu.make_async_copy(
            enc_h.at[:, pl.ds(pl.multiple_of(k * KB, KB), KB)], enc_v.at[k], in_sem.at[1 + k]
        )

    def dec_copy(n):
        return pltpu.make_async_copy(
            dec_h.at[:, pl.ds(pl.multiple_of(n * NB, NB), NB)], dec_v.at[n], in_sem.at[1 + NK + n]
        )

    for k in range(NK):
        enc_copy(k).start()
    c_bias = pltpu.make_async_copy(bias_h, bias, in_sem.at[1 + NK + NN])
    c_dbias = pltpu.make_async_copy(dbias_h, dbias, in_sem.at[2 + NK + NN])
    c_bias.start()
    c_dbias.start()

    barrier = pltpu.get_barrier_semaphore()
    pl.semaphore_signal(barrier, inc=1, device_id=partner, device_id_type=MESH)
    for o in range(1, Z):
        pl.semaphore_signal(barrier, inc=1, device_id=zdev(o), device_id_type=MESH)
    for o in range(1, NL):
        pl.semaphore_signal(barrier, inc=1, device_id=(w, lat_to(o)), device_id_type=MESH)

    def a1(h, k):
        return rc(stA.at[h, k, pc], rxA.at[h, k], a1s.at[h, k], a1r.at[h, k], partner)

    def a2(h, k, o):
        return rc(
            sA.at[h, k, (z + o) % Z], rA.at[h, k, o], a2s.at[h, k, o], a2r.at[h, k, o], zdev(o)
        )

    def own_z(ref, ssem, rsem):
        def send(h, k, o):
            block = ref.at[h, k, c, z]
            return rc(block, block, ssem.at[h, k, o], rsem.at[h, k, o], zdev(o))

        def arrive(h, k, o):
            block = ref.at[h, k, c, (z + Z - o) % Z]
            return rc(block, block, ssem.at[h, k, o], rsem.at[h, k, o], zdev(o))

        return send, arrive

    def own_core(ref, ssem, rsem):
        def send(h, k):
            block = ref.at[h, k, c]
            return rc(block, block, ssem.at[h, k], rsem.at[h, k], partner)

        def arrive(h, k):
            block = ref.at[h, k, pc]
            return rc(block, block, ssem.at[h, k], rsem.at[h, k], partner)

        return send, arrive

    a3, a3in = own_z(acts, a3s, a3r)
    a4, a4in = own_core(acts, a4s, a4r)
    d3, d3in = own_z(dp, d3s, d3r)
    d4, d4in = own_core(dp, d4s, d4r)

    def combine_a(h, k):
        a1(h, k).wait_recv()
        sA[h, k] = stA[h, k, c] + rxA[h, k]
        for o in range(1, Z):
            a2(h, k, o).start()

    c_res.wait()
    for n in range(NN):
        dec_copy(n).start()

    def pre_part(h, k):
        p = jnp.dot(res_v[h * TH:(h + 1) * TH, :], enc_v[k], preferred_element_type=F32)
        for j in range(2):
            stA[h, k, j] = p[:, j * KC:(j + 1) * KC].reshape(Z, TB, KC)

    def pre_early(k):
        enc_copy(k).wait()
        pre_part(0, k)

    def pre_first(k):
        enc_copy(k).wait()
        pre_part(0, k)
        a1(0, k).start()
        combine_a(0, k - EARLY)

    def pre_next(h, k):
        pre_part(h, k)
        a1(h, k).start()

    EARLY = NK // 2
    loop(EARLY, pre_early)
    pl.semaphore_wait(barrier, 1 + (Z - 1) + (NL - 1))
    loop(EARLY, lambda k: a1(0, k).start())
    lax.fori_loop(EARLY, NK, lambda k, _: (pre_first(k), 0)[1], 0)
    lax.fori_loop(NK - EARLY, NK, lambda k, _: (combine_a(0, k), 0)[1], 0)
    for h in range(1, H):
        loop(NK, lambda k: pre_next(h, k))
    c_bias.wait()
    c_dbias.wait()

    def fwd_a(h, k):
        for o in range(1, Z):
            a3in(h, k, o).wait_recv()
        a4(h, k).start()

    def act_step(h, k):
        for o in range(1, Z):
            a2(h, k, o).wait_recv()
        pre = sA[h, k, z]
        for o in range(1, Z):
            pre = pre + rA[h, k, o]
        pre = pre + bias[k, c]
        preS[h, k] = pre
        acts[h, k, c, z] = jnp.maximum(pre, 0.0).astype(BF16)
        for o in range(1, Z):
            a3(h, k, o).start()

    loop(NK, lambda k: act_step(0, k))
    loop(NK, lambda k: combine_a(1, k))

    def rt_step(n):
        rt_v[n] = res_v[:, pl.ds(pl.multiple_of(n * NB, NB), NB)].T

    loop(NN, rt_step)

    def b1(h, n, o):
        to = lat_to(o)
        return rc(sB.at[h, n, to], rB.at[h, n, o], bs.at[h, n, o], br.at[h, n, o], (w, to))

    def c1(h, n, o):
        block = err.at[h, n, l]
        return rc(block, block, cs.at[h, n, o], cr.at[h, n, o], (w, lat_to(o)))

    def c1in(h, n, o):
        block = err.at[h, n, lat_from(o)]
        return rc(block, block, cs.at[h, n, o], cr.at[h, n, o], (w, lat_to(o)))

    def rec_step(h, n):
        a = jnp.concatenate(
            [acts[h, k, j].reshape(TH, KC) for k in range(NK) for j in range(2)], axis=1
        )
        r = jnp.dot(a, dec_v[n], preferred_element_type=F32).reshape(NL, TL, NB)
        rf[h, n] = r
        sB[h, n] = r.astype(BF16)
        for o in range(1, NL):
            b1(h, n, o).start()

    def at_step(h, k):
        a = jnp.concatenate([acts[h, k, j].reshape(TH, KC) for j in range(2)], axis=1)
        actsT[h, k] = a.T

    def err_step(h, n):
        for o in range(1, NL):
            b1(h, n, o).wait_recv()
        r = rf[h, n, l]
        for o in range(1, NL):
            r = r + rB[h, n, o].astype(F32)
        own = res_v[
            pl.ds(pl.multiple_of(h * TH + l * TL, TL), TL),
            pl.ds(pl.multiple_of(n * NB, NB), NB),
        ]
        err[h, n, l] = (r + dbias[n] - own.astype(F32)).astype(BF16)
        for o in range(1, NL):
            c1(h, n, o).start()

    def recon(h):
        loop(NK, lambda k: fwd_a(h, k))
        if h == 0:
            for n in range(NN):
                dec_copy(n).wait()
        loop(NK, lambda k: a4in(h, k).wait_recv())
        loop(NN, lambda n: rec_step(h, n))
        loop(NK, lambda k: at_step(h, k))

    recon(0)

    def zero_step(k):
        for s in range(3):
            sacc[s, k] = jnp.zeros(sacc.shape[2:], F32)

    loop(NK, zero_step)

    def err_act(i):
        err_step(0, i)
        act_step(1, i)

    loop(NK, err_act)
    recon(1)

    def dec_rows(n, k):
        return dec_v[n, pl.ds(pl.multiple_of(k * KB, KB), KB), :]

    def dacts_part(h, n, k):
        d = lax.dot_general(
            err[h, n].reshape(TH, NB), dec_rows(n, k), NT, preferred_element_type=F32
        )
        return [d[:, j * KC:(j + 1) * KC].reshape(Z, TB, KC) for j in range(2)]

    def grad_first(n, k):
        grad[n, k] = jnp.dot(
            actsT[0, k], err[0, n].reshape(TH, NB), preferred_element_type=F32
        )

    def grad_last(n, k):
        g = grad[n, k] + jnp.dot(
            actsT[1, k], err[1, n].reshape(TH, NB), preferred_element_type=F32
        )
        grad[n, k] = g
        wt = dec_rows(n, k).astype(F32)
        for s, prod in enumerate((wt * wt, g * wt, g * g)):
            part = prod[:, 0:128]
            for j in range(1, NB // 128):
                part = part + prod[:, j * 128:(j + 1) * 128]
            sacc[s, k] += part

    def err_wait(h, n):
        for o in range(1, NL):
            c1in(h, n, o).wait_recv()

    def d1(h, k):
        return rc(sD.at[h, k, pc], rxD.at[h, k], d1s.at[h, k], d1r.at[h, k], partner)

    def d2(h, k, o):
        return rc(
            sS.at[h, k, (z + o) % Z], rD.at[h, k, o], d2s.at[h, k, o], d2r.at[h, k, o], zdev(o)
        )

    def combine_d(h, k):
        d1(h, k).wait_recv()
        s = dacc[h, k, c] + rxD[h, k].astype(F32)
        dacc[h, k, c] = s
        sS[h, k] = s.astype(BF16)
        for o in range(1, Z):
            d2(h, k, o).start()

    def dacts_add(h, n, k):
        for j, d in enumerate(dacts_part(h, n, k)):
            if isinstance(n, int) and n == 0:
                dacc[h, k, j] = d
            else:
                dacc[h, k, j] += d

    last = NN - 1

    def d_step(h, k):
        for j, d in enumerate(dacts_part(h, last, k)):
            v = dacc[h, k, j] + d
            dacc[h, k, j] = v
            sD[h, k, j] = v.astype(BF16)
        d1(h, k).start()

        @pl.when(k > 0)
        def _():
            combine_d(h, k - 1)

    def dacts(h, beside):
        def step(n):
            err_wait(h, n)

            def k_step(k):
                dacts_add(h, n, k)
                beside(n, k)

            loop(NK, k_step)

        step(0)
        lax.fori_loop(1, last, lambda n, _: (step(n), 0)[1], 0)
        err_wait(h, last)
        loop(NK, lambda k: d_step(h, k))
        combine_d(h, NK - 1)

    def dp_step(h, k):
        for o in range(1, Z):
            d2(h, k, o).wait_recv()
        v = dacc[h, k, c, z]
        for o in range(1, Z):
            v = v + rD[h, k, o].astype(F32)
        dp[h, k, c, z] = jnp.where(preS[h, k] > 0.0, v + PENALTY, 0.0).astype(BF16)
        for o in range(1, Z):
            d3(h, k, o).start()

    def fwd_d(h, k):
        for o in range(1, Z):
            d3in(h, k, o).wait_recv()
        d4(h, k).start()

    dacts(0, lambda n, k: None)

    def err_grad(i):
        err_step(1, i)
        loop(NK, lambda k: grad_first(i, k))

    loop(NN, err_grad)
    loop(NK, lambda k: dp_step(0, k))
    dacts(1, grad_last)

    def st_row(s, k, j):
        return (k * 3 + s) * (KB // 128) + j

    def gd_step(k):
        grad_last(last, k)
        for s in range(3):
            total = jnp.sum(sacc[s, k].T, axis=0, keepdims=True)
            for j in range(KB // 128):
                stv[pl.ds(st_row(s, k, j), 1), :] = total[:, j * 128:(j + 1) * 128]

    loop(NK, gd_step)

    e1 = rc(stv, rst, e1s, e1r, partner)
    e1.start()

    def e2(o):
        return rc(ss, rs2.at[o], e2s.at[o], e2r.at[o], zdev(o))

    loop(NK, lambda k: fwd_d(0, k))
    e1.wait_recv()
    ss[...] = stv[...] + rst[...]
    for o in range(1, Z):
        e2(o).start()
    loop(NK, lambda k: dp_step(1, k))
    for o in range(1, Z):
        e2(o).wait_recv()

    total = ss[...]
    for o in range(1, Z):
        total = total + rs2[o]
    st[...] = total

    def nd_step(k):
        ww, gw, gg = (
            jnp.concatenate(
                [st[pl.ds(st_row(s, k, j), 1), :] for j in range(KB // 128)], axis=1
            )
            for s in range(3)
        )
        coef = gw / (ww + EPS)
        sq = (
            ww
            - 2.0 * STEP * (gw - coef * ww)
            + STEP * STEP * (gg - 2.0 * coef * gw + coef * coef * ww)
        )
        inv = 1.0 / jnp.sqrt(sq + EPS)
        up = jnp.broadcast_to((1.0 + STEP * coef) * inv, (128, KB)).T
        down = jnp.broadcast_to(STEP * inv, (128, KB)).T
        for n in range(NN):
            for j in range(NB // 128):
                wt = dec_v[n, pl.ds(pl.multiple_of(k * KB, KB), KB), j * 128:(j + 1) * 128]
                g = grad[n, k, :, j * 128:(j + 1) * 128]
                first = n * NB + j * 128
                nd_v[k, :, first:first + 128] = (wt.astype(F32) * up - g * down).astype(BF16)

    loop(NK, nd_step)
    loop(NK, lambda k: fwd_d(1, k))
    for h in range(H):
        loop(NK, lambda k: d4in(h, k).wait_recv())

    def drain(k):
        for h in range(H):
            for first in (a1, a4, d1, d4):
                first(h, k).wait_send()
            for o in range(1, Z):
                for each in (a2, a3, d2, d3):
                    each(h, k, o).wait_send()

    def drain_n(n):
        for h in range(H):
            for o in range(1, NL):
                b1(h, n, o).wait_send()
                c1(h, n, o).wait_send()

    loop(NK, drain)
    loop(NN, drain_n)
    e1.wait_send()
    for o in range(1, Z):
        e2(o).wait_send()


def finish_kernel(rt, dp, nd, eg_o, nd_o, eg_v, sem):
    halves, blocks = dp.shape[:2]
    NN, NB = rt.shape[:2]
    NK, KB = nd.shape[:2]
    copies = [
        pltpu.make_async_copy(nd.at[k], nd_o.at[k * KB:(k + 1) * KB, :], sem.at[k])
        for k in range(NK)
    ]
    for copy in copies:
        copy.start()
    d = jnp.concatenate(
        [
            jnp.concatenate([dp[h, k] for k in range(blocks)], axis=1)
            for h in range(halves)
        ],
        axis=0,
    )
    for n in range(NN):
        eg_v[n] = jnp.dot(rt[n], d, preferred_element_type=F32).astype(BF16)
        copy = pltpu.make_async_copy(eg_v.at[n], eg_o.at[n * NB:(n + 1) * NB, :], sem.at[NK + n])
        copy.start()
        copies.append(copy)
    for copy in copies:
        copy.wait()


def fused(W, NL, residuals, encoder, enc_bias, decoder, dec_bias):
    T, DW = residuals.shape
    LL = encoder.shape[1]
    Z = W // 2
    NK, NN = 4, 4
    KB, NB = LL // NK, DW // NN
    H = 2
    TH = T // H
    TB, TL = TH // Z, TH // NL
    KC = KB // 2
    V = pltpu.VMEM
    dma = pltpu.SemaphoreType.DMA
    sums, part, rows = (H, NK, 2, Z, TB, KC), (H, NK, Z, TB, KC), (H, NN, NL, TL, NB)
    stats = (3 * LL // 128, 128)
    one, per_z, per_l = (H, NK), (H, NK, Z), (H, NN, NL)
    scratch = [
        V((T, DW), BF16), V((NK, DW, KB), BF16), V((NN, LL, NB), BF16),
        V((NK, 2, 1, KC), F32), V((NN, 1, NB), F32),
        V(sums, F32), V(part, F32), V(part, F32), V(part, F32), V((H, NK, TB, KC), F32),
        V(sums, BF16), V((H, NK, KB, TH), BF16),
        V(rows, F32), V(rows, BF16), V(rows, BF16), V(rows, BF16),
        V(sums, F32), V(sums, BF16), V(part, BF16), V(part, BF16), V(part, BF16),
        V((NN, NK, KB, NB), F32), V((3, NK, KB, 128), F32),
        V(stats, F32), V(stats, F32), V(stats, F32), V((Z, *stats), F32), V(stats, F32),
        dma((3 + NK + NN,)),
        dma(one), dma(one), dma(per_z), dma(per_z), dma(per_z), dma(per_z), dma(one), dma(one),
        dma(per_l), dma(per_l), dma(per_l), dma(per_l),
        dma(one), dma(one), dma(per_z), dma(per_z), dma(per_z), dma(per_z), dma(one), dma(one),
        dma, dma, dma((Z,)), dma((Z,)),
    ]
    hbm = pl.BlockSpec(memory_space=pltpu.HBM)
    vm = pl.BlockSpec(memory_space=pltpu.VMEM)
    new_decoder, dp, rt = pl.pallas_call(
        functools.partial(step_kernel, Z, NL, NK, NN),
        out_shape=(
            V((NK, KB, DW), BF16),
            V(sums, BF16),
            V((NN, NB, T), BF16),
        ),
        in_specs=[hbm] * 5,
        out_specs=(vm, vm, vm),
        scratch_shapes=scratch,
        compiler_params=pltpu.CompilerParams(
            collective_id=0, has_side_effects=True, vmem_limit_bytes=115 * 2**19
        ),
        name="sae_step",
    )(residuals, encoder, enc_bias.reshape(NK, 2, 1, KC), decoder, dec_bias.reshape(NN, 1, NB))
    return pl.pallas_call(
        finish_kernel,
        out_shape=(
            jax.ShapeDtypeStruct((DW, LL), BF16),
            jax.ShapeDtypeStruct((LL, DW), BF16),
        ),
        in_specs=[vm, vm, vm],
        out_specs=(hbm, hbm),
        scratch_shapes=[V((NN, NB, LL), BF16), dma((NK + NN,))],
        compiler_params=pltpu.CompilerParams(vmem_limit_bytes=30 * 2**20),
        cost_estimate=pl.CostEstimate(
            flops=2 * T * DW * LL, bytes_accessed=4 * DW * LL, transcendentals=0,
        ),
        name="finish",
    )(rt, dp.reshape(H, 2 * NK, TH, KC), new_decoder)


def plain(residuals, encoder, enc_bias, decoder, dec_bias):
    tokens = residuals.shape[0]
    lat_count = lax.axis_size("lat")
    lat_rows = tokens // lat_count
    rows = residuals
    pre_rows = (
        lax.psum_scatter(
            jnp.dot(rows, encoder, preferred_element_type=jnp.float32),
            "width",
            scatter_dimension=0,
            tiled=True,
        )
        + enc_bias
    )
    active_rows = pre_rows > 0.0
    act_rows = jnp.maximum(pre_rows, 0.0).astype(jnp.bfloat16)
    acts = lax.all_gather(act_rows, "width", axis=0, tiled=True)
    rows = acts
    recon_rows = lax.psum_scatter(
        jnp.dot(rows, decoder, preferred_element_type=jnp.float32),
        "lat",
        scatter_dimension=0,
        tiled=True,
    )
    first = lax.axis_index("lat") * lat_rows
    own_rows = lax.dynamic_slice_in_dim(residuals, first, lat_rows, 0)
    error_part = (recon_rows + dec_bias - own_rows.astype(jnp.float32)).astype(jnp.bfloat16)
    error = lax.all_gather(error_part, "lat", axis=0, tiled=True)
    rows = error
    dacts_rows = (
        lax.psum_scatter(
            lax.dot_general(
                rows, decoder, (((1,), (1,)), ((), ())), preferred_element_type=jnp.float32
            ),
            "width",
            scatter_dimension=0,
            tiled=True,
        )
        + PENALTY
    )
    dpre_part = jnp.where(active_rows, dacts_rows, 0.0).astype(jnp.bfloat16)
    dpre = lax.all_gather(dpre_part, "width", axis=0, tiled=True)
    enc_grad = lax.dot_general(
        residuals, dpre, (((0,), (0,)), ((), ())), preferred_element_type=jnp.float32
    ).astype(jnp.bfloat16)
    grad = lax.dot_general(
        acts, error, (((0,), (0,)), ((), ())), preferred_element_type=jnp.float32
    )
    weight = decoder.astype(jnp.float32)
    ww, gw, gg = lax.psum(
        (
            jnp.sum(weight * weight, axis=1),
            jnp.sum(grad * weight, axis=1),
            jnp.sum(grad * grad, axis=1),
        ),
        "width",
    )
    coef_row = gw / (ww + EPS)
    coef = coef_row[:, None]
    moved = weight - STEP * (grad - coef * weight)
    squared = (
        ww
        - 2.0 * STEP * (gw - coef_row * ww)
        + STEP * STEP * (gg - 2.0 * coef_row * gw + coef_row * coef_row * ww)
    )
    new_decoder = (moved / jnp.sqrt(squared + EPS)[:, None]).astype(jnp.bfloat16)
    return (enc_grad, new_decoder)


def per_device(W, NL, residuals, encoder, enc_bias, decoder, dec_bias):
    T, DW = residuals.shape
    LL = encoder.shape[1]
    args = (residuals, encoder, enc_bias, decoder, dec_bias)
    fits = W % 2 == 0 and NL % 2 == 0 and T % (16 * W) == 0 and T % (32 * NL) == 0
    if fits and DW % 512 == 0 and LL % 1024 == 0 and T % 128 == 0:
        return fused(W, NL, *args)
    return plain(*args)


def solution(mesh):
    return jax.shard_map(
        functools.partial(per_device, mesh.shape["width"], mesh.shape["lat"]),
        mesh=mesh,
        in_specs=(P(None, "width"), P("width", "lat"), P("lat"), P("lat", "width"), P("width")),
        out_specs=(P("width", "lat"), P("lat", "width")),
        check_vma=False,
    )
```

```python
import functools

import jax
import jax.numpy as jnp
from jax import lax
from jax.experimental import pallas as pl
from jax.experimental.pallas import tpu as pltpu
from jax.sharding import PartitionSpec as P

EPS = 1e-06
STEP = 0.0003
PENALTY = 0.5
MESH = pl.DeviceIdType.MESH
F32, BF16 = jnp.float32, jnp.bfloat16
NT = (((1,), (1,)), ((), ()))


def step_kernel(
    Z, NL, NK, NN,
    res_h, enc_h, bias_h, dec_h, dbias_h,
    nd_v, dp, rt_v,
    res_v, enc_v, dec_v, bias, dbias, stA, rxA, sA, qA, tA, rA, preS, acts, actsT,
    rf, sB, fB, tB, rB, err, dacc, sD, rxD, sS, rD, grad, sacc, stv, rst, ss, rs2, st,
    in_sem, sent,
    a1r, a2r, a3r, a4r, br, cr, d1r, d2r, d3r, d4r, e1r, e2r,
):
    T, DW = res_v.shape
    H = acts.shape[0]
    TH = T // H
    TB, KC = acts.shape[-2:]
    KB = 2 * KC
    TL, NB = err.shape[-2:]
    w = lax.axis_index("width")
    l = lax.axis_index("lat")
    z, c = w // 2, w % 2
    pc = 1 - c
    partner = (z * 2 + pc, l)

    side = z // 2
    near, far_in, far_out = z + 1 - 2 * (z % 2), 2 - side, 3 - 3 * side
    inner = (z + side) % 2

    def zdev(o):
        return ((z + o) % Z) * 2 + c, l

    def on(other):
        return other * 2 + c, l

    def lat_to(o):
        return ((l // 2 + o // 2) % (NL // 2)) * 2 + (l % 2 + o % 2) % 2

    lx, ly, ld = lat_to(1), lat_to(2), lat_to(3)

    def rc(src, dst, ssem, rsem, dev):
        return pltpu.make_async_remote_copy(
            src_ref=src, dst_ref=dst, send_sem=ssem, recv_sem=rsem,
            device_id=dev, device_id_type=MESH,
        )

    def arrived(ref, sem):
        rc(ref, ref, sem, sem, partner).wait_recv()

    def left(ref, sem):
        rc(ref, ref, sem, sem, partner).wait_send()

    A1, A2, A3, A4, B1, B2, C1, C2, D1, D2, D3, D4, E1, E2 = (
        sent.at[i] for i in range(14)
    )

    def span(first, stop, f):
        lax.fori_loop(first, stop, lambda i, _: (f(i), 0)[1], 0)

    def loop(n, f):
        lax.fori_loop(0, n, lambda i, _: (f(i), 0)[1], 0)

    c_res = pltpu.make_async_copy(res_h, res_v, in_sem.at[0])
    c_res.start()

    def enc_copy(k):
        return pltpu.make_async_copy(
            enc_h.at[:, pl.ds(pl.multiple_of(k * KB, KB), KB)], enc_v.at[k], in_sem.at[1 + k]
        )

    def dec_copy(n):
        return pltpu.make_async_copy(
            dec_h.at[:, pl.ds(pl.multiple_of(n * NB, NB), NB)], dec_v.at[n], in_sem.at[1 + NK + n]
        )

    for k in range(NK):
        enc_copy(k).start()
    c_bias = pltpu.make_async_copy(bias_h, bias, in_sem.at[1 + NK + NN])
    c_dbias = pltpu.make_async_copy(dbias_h, dbias, in_sem.at[2 + NK + NN])
    c_bias.start()
    c_dbias.start()

    barrier = pltpu.get_barrier_semaphore()
    pl.semaphore_signal(barrier, inc=1, device_id=partner, device_id_type=MESH)
    for o in range(1, Z):
        pl.semaphore_signal(barrier, inc=1, device_id=zdev(o), device_id_type=MESH)
    for o in range(1, NL):
        pl.semaphore_signal(barrier, inc=1, device_id=(w, lat_to(o)), device_id_type=MESH)

    def a1(h, k):
        return rc(stA.at[h, k, pc], rxA.at[h, k], A1, a1r.at[h, k], partner)

    def a2(h, k, i):
        src, dst, recv, to = (
            (sA.at[h, k, near], rA.at[h, k, 0], 0, near),
            (tA.at[h, k, 0], rA.at[h, k, 1], 0, far_in),
            (tA.at[h, k, 1], rA.at[h, k, 1], 0, far_out),
            (sA.at[h, k, far_in], qA.at[h, k, 0], 1, near),
            (sA.at[h, k, far_out], qA.at[h, k, 1], 1, near),
        )[i]
        return rc(src, dst, A2, a2r.at[h, k, recv], on(to))

    def a3(h, k, o):
        block = acts.at[h, k, c, z]
        return rc(block, block, A3, a3r.at[h, k], zdev(o))

    def d3(h, k, o):
        block = dp.at[h, k, c, z]
        return rc(block, block, D3, d3r.at[h, k], zdev(o))

    def own_core(ref, ssem, rsem):
        def send(h, k):
            block = ref.at[h, k, c]
            return rc(block, block, ssem, rsem.at[h, k], partner)

        def arrive(h, k):
            arrived(ref.at[h, k, pc], rsem.at[h, k])

        return send, arrive

    a4, a4in = own_core(acts, A4, a4r)
    d4, d4in = own_core(dp, D4, d4r)

    def combine_a(h, k):
        a1(h, k).wait_recv()
        sA[h, k] = stA[h, k, c] + rxA[h, k]

        @pl.when(inner == 0)
        def _():
            a2(h, k, 3).start()
            a2(h, k, 4).start()

        @pl.when(inner == 1)
        def _():
            a2(h, k, 0).start()

    def near_a(h, k):
        @pl.when(inner == 0)
        def _():
            a2(h, k, 0).start()

    def relay_a(h, k):
        @pl.when(inner == 1)
        def _():
            arrived(qA.at[h, k], a2r.at[h, k, 1])
            for i, block in enumerate((far_in, far_out)):
                tA[h, k, i] = sA[h, k, block] + qA[h, k, i]
                a2(h, k, 1 + i).start()

    c_res.wait()
    for n in range(NN):
        dec_copy(n).start()

    def pre_part(h, k):
        p = jnp.dot(res_v[h * TH:(h + 1) * TH, :], enc_v[k], preferred_element_type=F32)
        for j in range(2):
            stA[h, k, j] = p[:, j * KC:(j + 1) * KC].reshape(Z, TB, KC)

    def pre_early(k):
        enc_copy(k).wait()
        pre_part(0, k)

    def pre_first(k):
        enc_copy(k).wait()
        pre_part(0, k)
        a1(0, k).start()
        combine_a(0, k - EARLY)

    def pre_next(h, k):
        pre_part(h, k)
        a1(h, k).start()

    EARLY = NK // 2
    loop(EARLY, pre_early)
    pl.semaphore_wait(barrier, 1 + (Z - 1) + (NL - 1))
    loop(EARLY, lambda k: a1(0, k).start())
    lax.fori_loop(EARLY, NK, lambda k, _: (pre_first(k), 0)[1], 0)
    lax.fori_loop(NK - EARLY, NK, lambda k, _: (combine_a(0, k), 0)[1], 0)
    loop(NK, lambda k: near_a(0, k))
    for h in range(1, H):
        loop(NK, lambda k: pre_next(h, k))

    def second_a(k):
        combine_a(1, k)
        near_a(1, k)

    span(0, EARLY, second_a)
    c_bias.wait()
    c_dbias.wait()

    def fwd_a(h, k):
        arrived(acts.at[h, k, c, 1:Z], a3r.at[h, k])
        a4(h, k).start()

    def act_step(h, k):
        arrived(rA.at[h, k], a2r.at[h, k, 0])
        pre = (sA[h, k, z] + rA[h, k, 0]) + rA[h, k, 1]
        pre = pre + bias[k, c]
        preS[h, k] = pre
        acts[h, k, c, z] = jnp.maximum(pre, 0.0).astype(BF16)
        for o in range(1, Z):
            a3(h, k, o).start()

    loop(NK, lambda k: relay_a(0, k))
    loop(NK, lambda k: act_step(0, k))
    span(EARLY, NK, second_a)

    def rt_step(n):
        rt_v[n] = res_v[:, pl.ds(pl.multiple_of(n * NB, NB), NB)].T

    loop(NN, rt_step)
    span(0, EARLY, lambda k: relay_a(1, k))

    halves = (slice(0, NB // 2), slice(NB // 2, NB))

    def b1(h, n, i):
        to, block, half, dst = (
            (lx, ld, 1, fB.at[h, n, 0]),
            (ly, ld, 0, fB.at[h, n, 1]),
            (lx, lx, 1, rB.at[h, n, 0]),
            (ly, ly, 0, rB.at[h, n, 1]),
        )[i]
        return rc(sB.at[h, n, block, :, halves[half]], dst, B1, br.at[h, n, i // 2], (w, to))

    def b2(h, n, i):
        return rc(
            tB.at[h, n, i], rB.at[h, n, 2 + i], B2, br.at[h, n, 1], (w, (ly, lx)[i]),
        )

    def relay_b(h, n):
        arrived(fB.at[h, n], br.at[h, n, 0])
        for i, block, half in ((0, ly, 1), (1, lx, 0)):
            tB[h, n, i] = (rf[h, n, block, :, halves[half]] + fB[h, n, i].astype(F32)).astype(BF16)
            b2(h, n, i).start()

    def c1(h, n, i):
        block = err.at[h, n, l]
        return rc(block, block, C1, cr.at[h, n, 0], (w, (lx, ly)[i]))

    def c2(h, n, i):
        block = err.at[h, n, (lx, ly)[i], :, halves[1 - i]]
        return rc(block, block, C2, cr.at[h, n, 1], (w, (ly, lx)[i]))

    def fwd_c(h, n):
        arrived(err.at[h, n, 0:2], cr.at[h, n, 0])
        for i in range(2):
            c2(h, n, i).start()

    def rec_step(h, n):
        a = jnp.concatenate(
            [acts[h, k, j].reshape(TH, KC) for k in range(NK) for j in range(2)], axis=1
        )
        r = jnp.dot(a, dec_v[n], preferred_element_type=F32).reshape(NL, TL, NB)
        rf[h, n] = r
        sB[h, n] = r.astype(BF16)
        for i in range(4):
            b1(h, n, i).start()

    def at_step(h, k):
        a = jnp.concatenate([acts[h, k, j].reshape(TH, KC) for j in range(2)], axis=1)
        actsT[h, k] = a.T

    def err_step(h, n):
        arrived(rB.at[h, n], br.at[h, n, 1])
        for half in range(2):
            cols = halves[half]
            r = rf[h, n, l, :, cols]
            for j in (1 - half, 3 - half):
                r = r + rB[h, n, j].astype(F32)
            own = res_v[
                pl.ds(pl.multiple_of(h * TH + l * TL, TL), TL),
                pl.ds(pl.multiple_of(n * NB + half * (NB // 2), NB // 2), NB // 2),
            ]
            err[h, n, l, :, cols] = (r + dbias[n, :, cols] - own.astype(F32)).astype(BF16)
        for i in range(2):
            c1(h, n, i).start()

    loop(EARLY, lambda k: fwd_a(0, k))

    def fwd_relay(k):
        relay_a(1, k)
        fwd_a(0, k)

    span(EARLY, NK, fwd_relay)
    for n in range(NN):
        dec_copy(n).wait()
    loop(NK, lambda k: a4in(0, k))
    loop(NN, lambda n: rec_step(0, n))
    loop(NK, lambda k: act_step(1, k))
    loop(NK, lambda k: at_step(0, k))

    def zero_step(k):
        for s in range(3):
            sacc[s, k] = jnp.zeros(sacc.shape[2:], F32)

    loop(NK, zero_step)

    def rec_fwd(n):
        rec_step(1, n)
        fwd_c(0, n)

    loop(NN, lambda n: relay_b(0, n))
    span(0, NN // 2, lambda n: err_step(0, n))
    span(NN // 2, NN, lambda n: err_step(0, n))
    loop(NK, lambda k: fwd_a(1, k))
    loop(NK, lambda k: a4in(1, k))
    loop(NN, rec_fwd)
    loop(NK, lambda k: at_step(1, k))

    def dec_rows(n, k):
        return dec_v[n, pl.ds(pl.multiple_of(k * KB, KB), KB), :]

    def dacts_part(h, n, k):
        d = lax.dot_general(
            err[h, n].reshape(TH, NB), dec_rows(n, k), NT, preferred_element_type=F32
        )
        return [d[:, j * KC:(j + 1) * KC].reshape(Z, TB, KC) for j in range(2)]

    def grad_first(n, k):
        grad[n, k] = jnp.dot(
            actsT[0, k], err[0, n].reshape(TH, NB), preferred_element_type=F32
        )

    def grad_last(n, k):
        g = grad[n, k] + jnp.dot(
            actsT[1, k], err[1, n].reshape(TH, NB), preferred_element_type=F32
        )
        grad[n, k] = g
        wt = dec_rows(n, k).astype(F32)
        for s, prod in enumerate((wt * wt, g * wt, g * g)):
            part = prod[:, 0:128]
            for j in range(1, NB // 128):
                part = part + prod[:, j * 128:(j + 1) * 128]
            sacc[s, k] += part

    def err_wait(h, n):
        arrived(err.at[h, n, 0], cr.at[h, n, 1])

    def d1(h, k):
        return rc(sD.at[h, k, pc], rxD.at[h, k], D1, d1r.at[h, k], partner)

    def d2(h, k, o):
        return rc(
            sS.at[h, k, (z + o) % Z], rD.at[h, k, o], D2, d2r.at[h, k], zdev(o)
        )

    def combine_d(h, k):
        d1(h, k).wait_recv()
        s = dacc[h, k, c] + rxD[h, k].astype(F32)
        dacc[h, k, c] = s
        sS[h, k] = s.astype(BF16)
        for o in range(1, Z):
            d2(h, k, o).start()

    def dacts_add(h, n, k):
        for j, d in enumerate(dacts_part(h, n, k)):
            if isinstance(n, int) and n == 0:
                dacc[h, k, j] = d
            else:
                dacc[h, k, j] += d

    last = NN - 1

    def d_step(h, k):
        for j, d in enumerate(dacts_part(h, last, k)):
            v = dacc[h, k, j] + d
            dacc[h, k, j] = v
            sD[h, k, j] = v.astype(BF16)
        d1(h, k).start()

    def dacts(h, beside):
        def step(n):
            err_wait(h, n)

            def k_step(k):
                dacts_add(h, n, k)
                beside(n, k)

            loop(NK, k_step)

            if h == 0 and not isinstance(n, int):
                relay_b(1, n - 1)

        step(0)
        lax.fori_loop(1, last, lambda n, _: (step(n), 0)[1], 0)
        err_wait(h, last)
        if h == 0:
            relay_b(1, last - 1)
        loop(NK, lambda k: d_step(h, k))
        if h == 0:
            relay_b(1, last)
        loop(NK, lambda k: combine_d(h, k))

    def dp_step(h, k):
        arrived(rD.at[h, k, 1:Z], d2r.at[h, k])
        v = dacc[h, k, c, z]
        for o in range(1, Z):
            v = v + rD[h, k, o].astype(F32)
        dp[h, k, c, z] = jnp.where(preS[h, k] > 0.0, v + PENALTY, 0.0).astype(BF16)
        for o in range(1, Z):
            d3(h, k, o).start()

    def fwd_d(h, k):
        arrived(dp.at[h, k, c, 1:Z], d3r.at[h, k])
        d4(h, k).start()

    dacts(0, lambda n, k: None)

    def err_grad(i):
        err_step(1, i)
        loop(NK, lambda k: grad_first(i, k))

    loop(2, err_grad)
    for i in range(2, NN):
        err_grad(i)
        fwd_c(1, i - 2)
    fwd_c(1, NN - 2)
    loop(NK, lambda k: dp_step(0, k))
    fwd_c(1, NN - 1)
    dacts(1, grad_last)

    def st_row(s, k, j):
        return (k * 3 + s) * (KB // 128) + j

    def gd_step(k):
        grad_last(last, k)
        for s in range(3):
            total = jnp.sum(sacc[s, k].T, axis=0, keepdims=True)
            for j in range(KB // 128):
                stv[pl.ds(st_row(s, k, j), 1), :] = total[:, j * 128:(j + 1) * 128]

    loop(NK, gd_step)

    e1 = rc(stv, rst, E1, e1r, partner)
    e1.start()

    def e2(o):
        return rc(ss, rs2.at[o], E2, e2r, zdev(o))

    loop(NK, lambda k: fwd_d(0, k))
    e1.wait_recv()
    ss[...] = stv[...] + rst[...]
    for o in range(1, Z):
        e2(o).start()
    loop(NK, lambda k: dp_step(1, k))
    arrived(rs2.at[1:Z], e2r)

    total = ss[...]
    for o in range(1, Z):
        total = total + rs2[o]
    st[...] = total

    def nd_step(k):
        ww, gw, gg = (
            jnp.concatenate(
                [st[pl.ds(st_row(s, k, j), 1), :] for j in range(KB // 128)], axis=1
            )
            for s in range(3)
        )
        coef = gw / (ww + EPS)
        sq = (
            ww
            - 2.0 * STEP * (gw - coef * ww)
            + STEP * STEP * (gg - 2.0 * coef * gw + coef * coef * ww)
        )
        inv = 1.0 / jnp.sqrt(sq + EPS)
        up = jnp.broadcast_to((1.0 + STEP * coef) * inv, (128, KB)).T
        down = jnp.broadcast_to(STEP * inv, (128, KB)).T
        for n in range(NN):
            for j in range(NB // 128):
                wt = dec_v[n, pl.ds(pl.multiple_of(k * KB, KB), KB), j * 128:(j + 1) * 128]
                g = grad[n, k, :, j * 128:(j + 1) * 128]
                first = n * NB + j * 128
                nd_v[k, :, first:first + 128] = (wt.astype(F32) * up - g * down).astype(BF16)

    loop(NK, nd_step)
    loop(NK, lambda k: fwd_d(1, k))
    for h in range(H):
        loop(NK, lambda k: d4in(h, k))

    for ref, sem in (
        (rxA, A1), (sA.at[:, :, 1:Z], A2), (acts.at[:, :, 0, 1:Z], A3),
        (acts.at[:, :, 0], A4), (rB, B1), (tB, B2), (err.at[:, :, 0:2], C1), (err.at[:, :, 0], C2),
        (sD.at[:, :, 0], D1), (sS.at[:, :, 1:Z], D2), (dp.at[:, :, 0, 1:Z], D3),
        (dp.at[:, :, 0], D4), (ss, E1), (rs2.at[1:Z], E2),
    ):
        left(ref, sem)

def finish_kernel(rt, dp, nd, eg_o, nd_o, eg_v, sem):
    halves, blocks = dp.shape[:2]
    NN, NB = rt.shape[:2]
    NK, KB = nd.shape[:2]
    copies = [
        pltpu.make_async_copy(nd.at[k], nd_o.at[k * KB:(k + 1) * KB, :], sem.at[k])
        for k in range(NK)
    ]
    for copy in copies:
        copy.start()
    d = jnp.concatenate(
        [
            jnp.concatenate([dp[h, k] for k in range(blocks)], axis=1)
            for h in range(halves)
        ],
        axis=0,
    )
    for n in range(NN):
        eg_v[n] = jnp.dot(rt[n], d, preferred_element_type=F32).astype(BF16)
        copy = pltpu.make_async_copy(eg_v.at[n], eg_o.at[n * NB:(n + 1) * NB, :], sem.at[NK + n])
        copy.start()
        copies.append(copy)
    for copy in copies:
        copy.wait()


def fused(W, NL, residuals, encoder, enc_bias, decoder, dec_bias):
    T, DW = residuals.shape
    LL = encoder.shape[1]
    Z = W // 2
    NK, NN = 4, 4
    KB, NB = LL // NK, DW // NN
    H = 2
    TH = T // H
    TB, TL = TH // Z, TH // NL
    KC = KB // 2
    V = pltpu.VMEM
    dma = pltpu.SemaphoreType.DMA
    sums, part, rows = (H, NK, 2, Z, TB, KC), (H, NK, Z, TB, KC), (H, NN, NL, TL, NB)
    stats = (3 * LL // 128, 128)
    one, two = (H, NK), (H, NK, 2)
    half, pair = (TL, NB // 2), (H, NK, 2, TB, KC)
    scratch = [
        V((T, DW), BF16), V((NK, DW, KB), BF16), V((NN, LL, NB), BF16),
        V((NK, 2, 1, KC), F32), V((NN, 1, NB), F32),
        V(sums, F32), V(part, F32), V(part, F32), V(pair, F32), V(pair, F32), V(pair, F32),
        V((H, NK, TB, KC), F32),
        V(sums, BF16), V((H, NK, KB, TH), BF16),
        V(rows, F32), V(rows, BF16), V((H, NN, 2, *half), BF16), V((H, NN, 2, *half), BF16),
        V((H, NN, 4, *half), BF16), V(rows, BF16),
        V(sums, F32), V(sums, BF16), V(part, BF16), V(part, BF16), V(part, BF16),
        V((NN, NK, KB, NB), F32), V((3, NK, KB, 128), F32),
        V(stats, F32), V(stats, F32), V(stats, F32), V((Z, *stats), F32), V(stats, F32),
        dma((3 + NK + NN,)), dma((14,)),
        dma(one), dma(two), dma(one), dma(one), dma((H, NN, 2)), dma((H, NN, 2)),
        dma(one), dma(one), dma(one), dma(one), dma, dma,
    ]
    hbm = pl.BlockSpec(memory_space=pltpu.HBM)
    vm = pl.BlockSpec(memory_space=pltpu.VMEM)
    new_decoder, dp, rt = pl.pallas_call(
        functools.partial(step_kernel, Z, NL, NK, NN),
        out_shape=(
            V((NK, KB, DW), BF16),
            V(sums, BF16),
            V((NN, NB, T), BF16),
        ),
        in_specs=[hbm] * 5,
        out_specs=(vm, vm, vm),
        scratch_shapes=scratch,
        compiler_params=pltpu.CompilerParams(
            collective_id=0, has_side_effects=True, vmem_limit_bytes=115 * 2**19
        ),
        name="sae_step",
    )(residuals, encoder, enc_bias.reshape(NK, 2, 1, KC), decoder, dec_bias.reshape(NN, 1, NB))
    return pl.pallas_call(
        finish_kernel,
        out_shape=(
            jax.ShapeDtypeStruct((DW, LL), BF16),
            jax.ShapeDtypeStruct((LL, DW), BF16),
        ),
        in_specs=[vm, vm, vm],
        out_specs=(hbm, hbm),
        scratch_shapes=[V((NN, NB, LL), BF16), dma((NK + NN,))],
        compiler_params=pltpu.CompilerParams(vmem_limit_bytes=30 * 2**20),
        cost_estimate=pl.CostEstimate(
            flops=2 * T * DW * LL, bytes_accessed=4 * DW * LL, transcendentals=0,
        ),
        name="finish",
    )(rt, dp.reshape(H, 2 * NK, TH, KC), new_decoder)


def plain(residuals, encoder, enc_bias, decoder, dec_bias):
    tokens = residuals.shape[0]
    lat_count = lax.axis_size("lat")
    lat_rows = tokens // lat_count
    rows = residuals
    pre_rows = (
        lax.psum_scatter(
            jnp.dot(rows, encoder, preferred_element_type=jnp.float32),
            "width",
            scatter_dimension=0,
            tiled=True,
        )
        + enc_bias
    )
    active_rows = pre_rows > 0.0
    act_rows = jnp.maximum(pre_rows, 0.0).astype(jnp.bfloat16)
    acts = lax.all_gather(act_rows, "width", axis=0, tiled=True)
    rows = acts
    recon_rows = lax.psum_scatter(
        jnp.dot(rows, decoder, preferred_element_type=jnp.float32),
        "lat",
        scatter_dimension=0,
        tiled=True,
    )
    first = lax.axis_index("lat") * lat_rows
    own_rows = lax.dynamic_slice_in_dim(residuals, first, lat_rows, 0)
    error_part = (recon_rows + dec_bias - own_rows.astype(jnp.float32)).astype(jnp.bfloat16)
    error = lax.all_gather(error_part, "lat", axis=0, tiled=True)
    rows = error
    dacts_rows = (
        lax.psum_scatter(
            lax.dot_general(
                rows, decoder, (((1,), (1,)), ((), ())), preferred_element_type=jnp.float32
            ),
            "width",
            scatter_dimension=0,
            tiled=True,
        )
        + PENALTY
    )
    dpre_part = jnp.where(active_rows, dacts_rows, 0.0).astype(jnp.bfloat16)
    dpre = lax.all_gather(dpre_part, "width", axis=0, tiled=True)
    enc_grad = lax.dot_general(
        residuals, dpre, (((0,), (0,)), ((), ())), preferred_element_type=jnp.float32
    ).astype(jnp.bfloat16)
    grad = lax.dot_general(
        acts, error, (((0,), (0,)), ((), ())), preferred_element_type=jnp.float32
    )
    weight = decoder.astype(jnp.float32)
    ww, gw, gg = lax.psum(
        (
            jnp.sum(weight * weight, axis=1),
            jnp.sum(grad * weight, axis=1),
            jnp.sum(grad * grad, axis=1),
        ),
        "width",
    )
    coef_row = gw / (ww + EPS)
    coef = coef_row[:, None]
    moved = weight - STEP * (grad - coef * weight)
    squared = (
        ww
        - 2.0 * STEP * (gw - coef_row * ww)
        + STEP * STEP * (gg - 2.0 * coef_row * gw + coef_row * coef_row * ww)
    )
    new_decoder = (moved / jnp.sqrt(squared + EPS)[:, None]).astype(jnp.bfloat16)
    return (enc_grad, new_decoder)


def per_device(W, NL, residuals, encoder, enc_bias, decoder, dec_bias):
    T, DW = residuals.shape
    LL = encoder.shape[1]
    args = (residuals, encoder, enc_bias, decoder, dec_bias)
    fits = W == 8 and NL == 4 and T % (16 * W) == 0 and T % (32 * NL) == 0
    if fits and DW % 512 == 0 and LL % 1024 == 0 and T % 128 == 0:
        return fused(W, NL, *args)
    return plain(*args)


def solution(mesh):
    return jax.shard_map(
        functools.partial(per_device, mesh.shape["width"], mesh.shape["lat"]),
        mesh=mesh,
        in_specs=(P(None, "width"), P("width", "lat"), P("lat"), P("lat", "width"), P("width")),
        out_specs=(P("width", "lat"), P("lat", "width")),
        check_vma=False,
    )
```

```python
import functools

import jax
import jax.numpy as jnp
from jax import lax
from jax.experimental import pallas as pl
from jax.experimental.pallas import tpu as pltpu
from jax.sharding import PartitionSpec as P

EPS = 1e-06
STEP = 0.0003
PENALTY = 0.5
MESH = pl.DeviceIdType.MESH
F32, BF16 = jnp.float32, jnp.bfloat16
NT = (((1,), (1,)), ((), ()))


def step_kernel(
    Z, NL, NK, NN,
    res_h, enc_h, bias_h, dec_h, dbias_h,
    nd_v, dp, rt_v,
    res_v, enc_v, dec_v, bias, dbias, stA, rxA, sA, qA, tA, rA, preS, acts, actsT,
    rf, sB, fB, tB, rB, err, dacc, sD, rxD, sS, rD, grad, sacc, stv, rst, ss, rs2, st,
    in_sem, sent,
    a1r, a2r, a3r, a4r, br, cr, d1r, d2r, d3r, d4r, e1r, e2r,
):
    T, DW = res_v.shape
    H = acts.shape[0]
    TH = T // H
    TB, KC = acts.shape[-2:]
    KB = 2 * KC
    TL, NB = err.shape[-2:]
    w = lax.axis_index("width")
    l = lax.axis_index("lat")
    z, c = w // 2, w % 2
    pc = 1 - c
    partner = (z * 2 + pc, l)

    side = z // 2
    near, far_in, far_out = z + 1 - 2 * (z % 2), 2 - side, 3 - 3 * side
    inner = (z + side) % 2

    def zdev(o):
        return ((z + o) % Z) * 2 + c, l

    def on(other):
        return other * 2 + c, l

    def lat_to(o):
        return ((l // 2 + o // 2) % (NL // 2)) * 2 + (l % 2 + o % 2) % 2

    lx, ly, ld = lat_to(1), lat_to(2), lat_to(3)

    def rc(src, dst, ssem, rsem, dev):
        return pltpu.make_async_remote_copy(
            src_ref=src, dst_ref=dst, send_sem=ssem, recv_sem=rsem,
            device_id=dev, device_id_type=MESH,
        )

    def arrived(ref, sem):
        rc(ref, ref, sem, sem, partner).wait_recv()

    def left(ref, sem):
        rc(ref, ref, sem, sem, partner).wait_send()

    A1, A2, A3, A4, B1, B2, C1, C2, D1, D2, D3, D4, E1, E2 = (
        sent.at[i] for i in range(14)
    )

    def span(first, stop, f):
        lax.fori_loop(first, stop, lambda i, _: (f(i), 0)[1], 0)

    def loop(n, f):
        lax.fori_loop(0, n, lambda i, _: (f(i), 0)[1], 0)

    c_res = pltpu.make_async_copy(res_h, res_v, in_sem.at[0])
    c_res.start()

    def enc_copy(k):
        return pltpu.make_async_copy(
            enc_h.at[:, pl.ds(pl.multiple_of(k * KB, KB), KB)], enc_v.at[k], in_sem.at[1 + k]
        )

    def dec_copy(n):
        return pltpu.make_async_copy(
            dec_h.at[:, pl.ds(pl.multiple_of(n * NB, NB), NB)], dec_v.at[n], in_sem.at[1 + NK + n]
        )

    for k in range(NK):
        enc_copy(k).start()
    c_bias = pltpu.make_async_copy(bias_h, bias, in_sem.at[1 + NK + NN])
    c_dbias = pltpu.make_async_copy(dbias_h, dbias, in_sem.at[2 + NK + NN])
    c_bias.start()
    c_dbias.start()

    barrier = pltpu.get_barrier_semaphore()
    pl.semaphore_signal(barrier, inc=1, device_id=partner, device_id_type=MESH)
    for o in range(1, Z):
        pl.semaphore_signal(barrier, inc=1, device_id=zdev(o), device_id_type=MESH)
    for o in range(1, NL):
        pl.semaphore_signal(barrier, inc=1, device_id=(w, lat_to(o)), device_id_type=MESH)

    def a1(h, k):
        return rc(stA.at[h, k, pc], rxA.at[h, k], A1, a1r.at[h, k], partner)

    def a2(h, k, i):
        src, dst, recv, to = (
            (sA.at[h, k, near], rA.at[h, k, 0], 0, near),
            (tA.at[h, k, 0], rA.at[h, k, 1], 0, far_in),
            (tA.at[h, k, 1], rA.at[h, k, 1], 0, far_out),
            (sA.at[h, k, far_in], qA.at[h, k, 0], 1, near),
            (sA.at[h, k, far_out], qA.at[h, k, 1], 1, near),
        )[i]
        return rc(src, dst, A2, a2r.at[h, k, recv], on(to))

    def a3(h, k, o):
        block = acts.at[h, k, c, z]
        return rc(block, block, A3, a3r.at[h, k], zdev(o))

    def d3(h, k, o):
        block = dp.at[h, k, c, z]
        return rc(block, block, D3, d3r.at[h, k], zdev(o))

    def own_core(ref, ssem, rsem):
        def send(h, k):
            block = ref.at[h, k, c]
            return rc(block, block, ssem, rsem.at[h, k], partner)

        def arrive(h, k):
            arrived(ref.at[h, k, pc], rsem.at[h, k])

        return send, arrive

    a4, a4in = own_core(acts, A4, a4r)
    d4, d4in = own_core(dp, D4, d4r)

    def combine_a(h, k):
        a1(h, k).wait_recv()
        sA[h, k] = stA[h, k, c] + rxA[h, k]

        @pl.when(inner == 0)
        def _():
            a2(h, k, 3).start()
            a2(h, k, 4).start()

        @pl.when(inner == 1)
        def _():
            a2(h, k, 0).start()

    def near_a(h, k):
        @pl.when(inner == 0)
        def _():
            a2(h, k, 0).start()

    def relay_a(h, k):
        @pl.when(inner == 1)
        def _():
            arrived(qA.at[h, k], a2r.at[h, k, 1])
            for i, block in enumerate((far_in, far_out)):
                tA[h, k, i] = sA[h, k, block] + qA[h, k, i]
                a2(h, k, 1 + i).start()

    c_res.wait()
    for n in range(NN):
        dec_copy(n).start()

    def pre_part(h, k):
        p = jnp.dot(res_v[h * TH:(h + 1) * TH, :], enc_v[k], preferred_element_type=F32)
        for j in range(2):
            stA[h, k, j] = p[:, j * KC:(j + 1) * KC].reshape(Z, TB, KC)

    def pre_early(k):
        enc_copy(k).wait()
        pre_part(0, k)

    def pre_first(k):
        enc_copy(k).wait()
        pre_part(0, k)
        a1(0, k).start()
        combine_a(0, k - EARLY)

    def pre_next(h, k):
        pre_part(h, k)
        a1(h, k).start()

    EARLY = NK // 2
    loop(EARLY, pre_early)
    pl.semaphore_wait(barrier, 1 + (Z - 1) + (NL - 1))
    loop(EARLY, lambda k: a1(0, k).start())
    lax.fori_loop(EARLY, NK, lambda k, _: (pre_first(k), 0)[1], 0)
    lax.fori_loop(NK - EARLY, NK, lambda k, _: (combine_a(0, k), 0)[1], 0)
    loop(NK, lambda k: near_a(0, k))
    def second_a(h, k):
        combine_a(h, k)
        near_a(h, k)

    loop(NK, lambda k: pre_next(1, k))
    loop(NK, lambda k: second_a(1, k))
    loop(NK, lambda k: pre_next(2, k))
    c_bias.wait()
    c_dbias.wait()

    def fwd_a(h, k):
        arrived(acts.at[h, k, c, 1:Z], a3r.at[h, k])
        a4(h, k).start()

    def act_step(h, k):
        arrived(rA.at[h, k], a2r.at[h, k, 0])
        pre = (sA[h, k, z] + rA[h, k, 0]) + rA[h, k, 1]
        pre = pre + bias[k, c]
        preS[h, k] = pre
        acts[h, k, c, z] = jnp.maximum(pre, 0.0).astype(BF16)
        for o in range(1, Z):
            a3(h, k, o).start()

    loop(NK, lambda k: relay_a(0, k))
    loop(NK, lambda k: act_step(0, k))
    loop(NK, lambda k: second_a(2, k))

    def rt_step(n):
        rt_v[n] = res_v[:, pl.ds(pl.multiple_of(n * NB, NB), NB)].T

    loop(NN, rt_step)
    loop(NK, lambda k: relay_a(1, k))

    halves = (slice(0, NB // 2), slice(NB // 2, NB))

    def b1(h, n, i):
        to, block, half, dst = (
            (lx, ld, 1, fB.at[h, n, 0]),
            (ly, ld, 0, fB.at[h, n, 1]),
            (lx, lx, 1, rB.at[h, n, 0]),
            (ly, ly, 0, rB.at[h, n, 1]),
        )[i]
        return rc(sB.at[h, n, block, :, halves[half]], dst, B1, br.at[h, n, i // 2], (w, to))

    def b2(h, n, i):
        return rc(
            tB.at[h, n, i], rB.at[h, n, 2 + i], B2, br.at[h, n, 1], (w, (ly, lx)[i]),
        )

    def relay_b(h, n):
        arrived(fB.at[h, n], br.at[h, n, 0])
        for i, block, half in ((0, ly, 1), (1, lx, 0)):
            tB[h, n, i] = (rf[h, n, block, :, halves[half]] + fB[h, n, i].astype(F32)).astype(BF16)
            b2(h, n, i).start()

    def c1(h, n, i):
        block = err.at[h, n, l]
        return rc(block, block, C1, cr.at[h, n, 0], (w, (lx, ly)[i]))

    def c2(h, n, i):
        block = err.at[h, n, (lx, ly)[i], :, halves[1 - i]]
        return rc(block, block, C2, cr.at[h, n, 1], (w, (ly, lx)[i]))

    def fwd_c(h, n):
        arrived(err.at[h, n, 0:2], cr.at[h, n, 0])
        for i in range(2):
            c2(h, n, i).start()

    def rec_step(h, n):
        a = jnp.concatenate(
            [acts[h, k, j].reshape(TH, KC) for k in range(NK) for j in range(2)], axis=1
        )
        r = jnp.dot(a, dec_v[n], preferred_element_type=F32).reshape(NL, TL, NB)
        rf[h, n] = r
        sB[h, n] = r.astype(BF16)
        for i in range(4):
            b1(h, n, i).start()

    def at_step(h, k):
        a = jnp.concatenate([acts[h, k, j].reshape(TH, KC) for j in range(2)], axis=1)
        actsT[k, :, h * TH:(h + 1) * TH] = a.T

    def err_step(h, n):
        arrived(rB.at[h, n], br.at[h, n, 1])
        for half in range(2):
            cols = halves[half]
            r = rf[h, n, l, :, cols]
            for j in (1 - half, 3 - half):
                r = r + rB[h, n, j].astype(F32)
            own = res_v[
                pl.ds(pl.multiple_of(h * TH + l * TL, TL), TL),
                pl.ds(pl.multiple_of(n * NB + half * (NB // 2), NB // 2), NB // 2),
            ]
            err[h, n, l, :, cols] = (r + dbias[n, :, cols] - own.astype(F32)).astype(BF16)
        for i in range(2):
            c1(h, n, i).start()

    loop(NK, lambda k: fwd_a(0, k))
    for n in range(NN):
        dec_copy(n).wait()
    loop(NK, lambda k: a4in(0, k))
    loop(NN, lambda n: rec_step(0, n))
    loop(NK, lambda k: act_step(1, k))
    loop(NK, lambda k: relay_a(2, k))
    loop(NK, lambda k: at_step(0, k))

    def zero_step(k):
        for s in range(3):
            sacc[s, k] = jnp.zeros(sacc.shape[2:], F32)

    loop(NK, zero_step)

    loop(NN, lambda n: relay_b(0, n))
    loop(NN, lambda n: err_step(0, n))
    loop(NK, lambda k: fwd_a(1, k))
    loop(NK, lambda k: a4in(1, k))
    loop(NN, lambda n: rec_step(1, n))
    loop(NK, lambda k: act_step(2, k))
    loop(NN, lambda n: fwd_c(0, n))
    loop(NK, lambda k: at_step(1, k))
    loop(NN, lambda n: relay_b(1, n))

    def dec_rows(n, k):
        return dec_v[n, pl.ds(pl.multiple_of(k * KB, KB), KB), :]

    def dacts_part(h, n, k):
        d = lax.dot_general(
            err[h, n].reshape(TH, NB), dec_rows(n, k), NT, preferred_element_type=F32
        )
        return [d[:, j * KC:(j + 1) * KC].reshape(Z, TB, KC) for j in range(2)]

    def grad_first(n, k):
        grad[n, k] = jnp.dot(
            actsT[k, :, 0:2 * TH], err[0:2, n].reshape(2 * TH, NB), preferred_element_type=F32
        )

    def grad_last(n, k):
        g = grad[n, k] + jnp.dot(
            actsT[k, :, 2 * TH:T], err[2, n].reshape(TH, NB), preferred_element_type=F32
        )
        grad[n, k] = g
        wt = dec_rows(n, k).astype(F32)
        for s, prod in enumerate((wt * wt, g * wt, g * g)):
            part = prod[:, 0:128]
            for j in range(1, NB // 128):
                part = part + prod[:, j * 128:(j + 1) * 128]
            sacc[s, k] += part

    def err_wait(h, n):
        arrived(err.at[h, n, 0], cr.at[h, n, 1])

    def d1(h, k):
        return rc(sD.at[h, k, pc], rxD.at[h, k], D1, d1r.at[h, k], partner)

    def d2(h, k, o):
        return rc(
            sS.at[h, k, (z + o) % Z], rD.at[h, k, o], D2, d2r.at[h, k], zdev(o)
        )

    def combine_d(h, k):
        d1(h, k).wait_recv()
        s = dacc[h, k, c] + rxD[h, k].astype(F32)
        dacc[h, k, c] = s
        sS[h, k] = s.astype(BF16)
        for o in range(1, Z):
            d2(h, k, o).start()

    def dacts_add(h, n, k):
        for j, d in enumerate(dacts_part(h, n, k)):
            if isinstance(n, int) and n == 0:
                dacc[h, k, j] = d
            else:
                dacc[h, k, j] += d

    last = NN - 1

    def d_step(h, k):
        for j, d in enumerate(dacts_part(h, last, k)):
            v = dacc[h, k, j] + d
            dacc[h, k, j] = v
            sD[h, k, j] = v.astype(BF16)
        d1(h, k).start()

    def dacts(h, n):
        err_wait(h, n)
        for k in range(NK):
            dacts_add(h, n, k)

    def d_steps(h):
        err_wait(h, last)
        for k in range(NK):
            d_step(h, k)

    def dp_step(h, k):
        arrived(rD.at[h, k, 1:Z], d2r.at[h, k])
        v = dacc[h, k, c, z]
        for o in range(1, Z):
            v = v + rD[h, k, o].astype(F32)
        dp[h, k, c, z] = jnp.where(preS[h, k] > 0.0, v + PENALTY, 0.0).astype(BF16)
        for o in range(1, Z):
            d3(h, k, o).start()

    def fwd_d(h, k):
        arrived(dp.at[h, k, c, 1:Z], d3r.at[h, k])
        d4(h, k).start()

    def grad_n(n):
        for k in range(NK):
            grad_first(n, k)

    def err_dacts(n):
        err_step(2, n)
        dacts(1, n)

    loop(NK, lambda k: fwd_a(2, k))
    err_step(1, 0)
    dacts(0, 0)
    err_step(1, 1)
    loop(NK, lambda k: a4in(2, k))

    def err_rec(n):
        rec_step(2, n - NN // 2)
        err_step(1, n)

    span(NN // 2, NN, err_rec)
    span(NN - NN // 2, NN, lambda n: rec_step(2, n))

    def dacts_fwd(n):
        dacts(0, n)
        fwd_c(1, n - 1)

    span(1, last, dacts_fwd)
    d_steps(0)
    span(NN - 2, NN, lambda n: fwd_c(1, n))
    loop(NK, lambda k: combine_d(0, k))
    relay_b(2, 0)
    loop(NK, lambda k: at_step(2, k))
    span(1, NN, lambda n: relay_b(2, n))
    err_dacts(0)
    span(1, last, err_dacts)
    err_step(2, last)
    d_steps(1)
    fwd_c(2, 0)
    loop(NK, lambda k: dp_step(0, k))
    loop(NK, lambda k: combine_d(1, k))
    fwd_c(2, 1)
    grad_n(0)
    fwd_c(2, 2)
    grad_n(1)
    fwd_c(2, 3)
    grad_n(2)
    dacts(2, 0)
    grad_n(3)
    span(1, last, lambda n: dacts(2, n))
    d_steps(2)
    loop(NK, lambda k: combine_d(2, k))
    loop(NK, lambda k: dp_step(1, k))

    def grads_last(n):
        for k in range(NK):
            grad_last(n, k)

    span(0, last, grads_last)

    def st_row(s, k, j):
        return (k * 3 + s) * (KB // 128) + j

    def gd_step(k):
        grad_last(last, k)
        for s in range(3):
            total = jnp.sum(sacc[s, k].T, axis=0, keepdims=True)
            for j in range(KB // 128):
                stv[pl.ds(st_row(s, k, j), 1), :] = total[:, j * 128:(j + 1) * 128]

    for k in range(NK):
        gd_step(k)

    e1 = rc(stv, rst, E1, e1r, partner)
    e1.start()

    def e2(o):
        return rc(ss, rs2.at[o], E2, e2r, zdev(o))

    loop(NK, lambda k: fwd_d(0, k))
    e1.wait_recv()
    ss[...] = stv[...] + rst[...]
    for o in range(1, Z):
        e2(o).start()
    loop(NK, lambda k: dp_step(2, k))
    loop(NK, lambda k: fwd_d(1, k))
    arrived(rs2.at[1:Z], e2r)

    total = ss[...]
    for o in range(1, Z):
        total = total + rs2[o]
    st[...] = total

    def nd_step(k):
        ww, gw, gg = (
            jnp.concatenate(
                [st[pl.ds(st_row(s, k, j), 1), :] for j in range(KB // 128)], axis=1
            )
            for s in range(3)
        )
        coef = gw / (ww + EPS)
        sq = (
            ww
            - 2.0 * STEP * (gw - coef * ww)
            + STEP * STEP * (gg - 2.0 * coef * gw + coef * coef * ww)
        )
        inv = 1.0 / jnp.sqrt(sq + EPS)
        up = jnp.broadcast_to((1.0 + STEP * coef) * inv, (128, KB)).T
        down = jnp.broadcast_to(STEP * inv, (128, KB)).T
        for n in range(NN):
            for j in range(NB // 128):
                wt = dec_v[n, pl.ds(pl.multiple_of(k * KB, KB), KB), j * 128:(j + 1) * 128]
                g = grad[n, k, :, j * 128:(j + 1) * 128]
                first = n * NB + j * 128
                nd_v[k, :, first:first + 128] = (wt.astype(F32) * up - g * down).astype(BF16)

    loop(NK, nd_step)
    loop(NK, lambda k: fwd_d(2, k))
    for h in range(H):
        loop(NK, lambda k: d4in(h, k))

    for ref, sem in (
        (rxA, A1), (sA.at[:, :, 1:Z], A2), (acts.at[:, :, 0, 1:Z], A3),
        (acts.at[:, :, 0], A4), (rB, B1), (tB, B2), (err.at[:, :, 0:2], C1), (err.at[:, :, 0], C2),
        (sD.at[:, :, 0], D1), (sS.at[:, :, 1:Z], D2), (dp.at[:, :, 0, 1:Z], D3),
        (dp.at[:, :, 0], D4), (ss, E1), (rs2.at[1:Z], E2),
    ):
        left(ref, sem)

def finish_kernel(rt, dp, nd, eg_o, nd_o, eg_v, sem):
    halves, blocks = dp.shape[:2]
    NN, NB = rt.shape[:2]
    NK, KB = nd.shape[:2]
    copies = [
        pltpu.make_async_copy(nd.at[k], nd_o.at[k * KB:(k + 1) * KB, :], sem.at[k])
        for k in range(NK)
    ]
    for copy in copies:
        copy.start()
    d = jnp.concatenate(
        [
            jnp.concatenate([dp[h, k] for k in range(blocks)], axis=1)
            for h in range(halves)
        ],
        axis=0,
    )
    for n in range(NN):
        eg_v[n] = jnp.dot(rt[n], d, preferred_element_type=F32).astype(BF16)
        copy = pltpu.make_async_copy(eg_v.at[n], eg_o.at[n * NB:(n + 1) * NB, :], sem.at[NK + n])
        copy.start()
        copies.append(copy)
    for copy in copies:
        copy.wait()


def fused(W, NL, residuals, encoder, enc_bias, decoder, dec_bias):
    T, DW = residuals.shape
    LL = encoder.shape[1]
    Z = W // 2
    NK, NN = 4, 4
    KB, NB = LL // NK, DW // NN
    H = 3
    TH = T // H
    TB, TL = TH // Z, TH // NL
    KC = KB // 2
    V = pltpu.VMEM
    dma = pltpu.SemaphoreType.DMA
    sums, part, rows = (H, NK, 2, Z, TB, KC), (H, NK, Z, TB, KC), (H, NN, NL, TL, NB)
    stats = (3 * LL // 128, 128)
    one, two = (H, NK), (H, NK, 2)
    half, pair = (TL, NB // 2), (H, NK, 2, TB, KC)
    scratch = [
        V((T, DW), BF16), V((NK, DW, KB), BF16), V((NN, LL, NB), BF16),
        V((NK, 2, 1, KC), F32), V((NN, 1, NB), F32),
        V(sums, F32), V(part, F32), V(part, F32), V(pair, F32), V(pair, F32), V(pair, F32),
        V((H, NK, TB, KC), F32),
        V(sums, BF16), V((NK, KB, T), BF16),
        V(rows, F32), V(rows, BF16), V((H, NN, 2, *half), BF16), V((H, NN, 2, *half), BF16),
        V((H, NN, 4, *half), BF16), V(rows, BF16),
        V(sums, F32), V(sums, BF16), V(part, BF16), V(part, BF16), V(part, BF16),
        V((NN, NK, KB, NB), F32), V((3, NK, KB, 128), F32),
        V(stats, F32), V(stats, F32), V(stats, F32), V((Z, *stats), F32), V(stats, F32),
        dma((3 + NK + NN,)), dma((14,)),
        dma(one), dma(two), dma(one), dma(one), dma((H, NN, 2)), dma((H, NN, 2)),
        dma(one), dma(one), dma(one), dma(one), dma, dma,
    ]
    hbm = pl.BlockSpec(memory_space=pltpu.HBM)
    vm = pl.BlockSpec(memory_space=pltpu.VMEM)
    new_decoder, dp, rt = pl.pallas_call(
        functools.partial(step_kernel, Z, NL, NK, NN),
        out_shape=(
            V((NK, KB, DW), BF16),
            V(sums, BF16),
            V((NN, NB, T), BF16),
        ),
        in_specs=[hbm] * 5,
        out_specs=(vm, vm, vm),
        scratch_shapes=scratch,
        compiler_params=pltpu.CompilerParams(
            collective_id=0, has_side_effects=True, vmem_limit_bytes=115 * 2**19
        ),
        name="sae_step",
    )(residuals, encoder, enc_bias.reshape(NK, 2, 1, KC), decoder, dec_bias.reshape(NN, 1, NB))
    return pl.pallas_call(
        finish_kernel,
        out_shape=(
            jax.ShapeDtypeStruct((DW, LL), BF16),
            jax.ShapeDtypeStruct((LL, DW), BF16),
        ),
        in_specs=[vm, vm, vm],
        out_specs=(hbm, hbm),
        scratch_shapes=[V((NN, NB, LL), BF16), dma((NK + NN,))],
        compiler_params=pltpu.CompilerParams(vmem_limit_bytes=30 * 2**20),
        cost_estimate=pl.CostEstimate(
            flops=2 * T * DW * LL, bytes_accessed=4 * DW * LL, transcendentals=0,
        ),
        name="finish",
    )(rt, dp.reshape(H, 2 * NK, TH, KC), new_decoder)


def plain(residuals, encoder, enc_bias, decoder, dec_bias):
    tokens = residuals.shape[0]
    lat_count = lax.axis_size("lat")
    lat_rows = tokens // lat_count
    rows = residuals
    pre_rows = (
        lax.psum_scatter(
            jnp.dot(rows, encoder, preferred_element_type=jnp.float32),
            "width",
            scatter_dimension=0,
            tiled=True,
        )
        + enc_bias
    )
    active_rows = pre_rows > 0.0
    act_rows = jnp.maximum(pre_rows, 0.0).astype(jnp.bfloat16)
    acts = lax.all_gather(act_rows, "width", axis=0, tiled=True)
    rows = acts
    recon_rows = lax.psum_scatter(
        jnp.dot(rows, decoder, preferred_element_type=jnp.float32),
        "lat",
        scatter_dimension=0,
        tiled=True,
    )
    first = lax.axis_index("lat") * lat_rows
    own_rows = lax.dynamic_slice_in_dim(residuals, first, lat_rows, 0)
    error_part = (recon_rows + dec_bias - own_rows.astype(jnp.float32)).astype(jnp.bfloat16)
    error = lax.all_gather(error_part, "lat", axis=0, tiled=True)
    rows = error
    dacts_rows = (
        lax.psum_scatter(
            lax.dot_general(
                rows, decoder, (((1,), (1,)), ((), ())), preferred_element_type=jnp.float32
            ),
            "width",
            scatter_dimension=0,
            tiled=True,
        )
        + PENALTY
    )
    dpre_part = jnp.where(active_rows, dacts_rows, 0.0).astype(jnp.bfloat16)
    dpre = lax.all_gather(dpre_part, "width", axis=0, tiled=True)
    enc_grad = lax.dot_general(
        residuals, dpre, (((0,), (0,)), ((), ())), preferred_element_type=jnp.float32
    ).astype(jnp.bfloat16)
    grad = lax.dot_general(
        acts, error, (((0,), (0,)), ((), ())), preferred_element_type=jnp.float32
    )
    weight = decoder.astype(jnp.float32)
    ww, gw, gg = lax.psum(
        (
            jnp.sum(weight * weight, axis=1),
            jnp.sum(grad * weight, axis=1),
            jnp.sum(grad * grad, axis=1),
        ),
        "width",
    )
    coef_row = gw / (ww + EPS)
    coef = coef_row[:, None]
    moved = weight - STEP * (grad - coef * weight)
    squared = (
        ww
        - 2.0 * STEP * (gw - coef_row * ww)
        + STEP * STEP * (gg - 2.0 * coef_row * gw + coef_row * coef_row * ww)
    )
    new_decoder = (moved / jnp.sqrt(squared + EPS)[:, None]).astype(jnp.bfloat16)
    return (enc_grad, new_decoder)


def per_device(W, NL, residuals, encoder, enc_bias, decoder, dec_bias):
    T, DW = residuals.shape
    LL = encoder.shape[1]
    args = (residuals, encoder, enc_bias, decoder, dec_bias)
    fits = W == 8 and NL == 4 and T % (48 * NL) == 0
    if fits and DW % 512 == 0 and LL % 1024 == 0 and T % 128 == 0:
        return fused(W, NL, *args)
    return plain(*args)


def solution(mesh):
    return jax.shard_map(
        functools.partial(per_device, mesh.shape["width"], mesh.shape["lat"]),
        mesh=mesh,
        in_specs=(P(None, "width"), P("width", "lat"), P("lat"), P("lat", "width"), P("width")),
        out_specs=(P("width", "lat"), P("lat", "width")),
        check_vma=False,
    )
```

```python
import functools

import jax
import jax.numpy as jnp
from jax import lax
from jax.experimental import pallas as pl
from jax.experimental.pallas import tpu as pltpu
from jax.sharding import PartitionSpec as P

EPS = 1e-06
STEP = 0.0003
PENALTY = 0.5
MESH = pl.DeviceIdType.MESH
F32, BF16 = jnp.float32, jnp.bfloat16
NT = (((1,), (1,)), ((), ()))


def step_kernel(
    Z, NL, NK, NN,
    res_h, enc_h, bias_h, dec_h, dbias_h,
    nd_v, dp, rt_v,
    res_v, enc_v, dec_v, bias, dbias, stA, rxA, sA, qA, tA, rA, preS, acts, actsT,
    rf, sB, fB, tB, rB, err, dacc, sD, rxD, sS, rD, grad, sacc, stv, rst, ss, rs2, st,
    in_sem, sent,
    r1, r2, r3, r4, rx, e1r, e2r,
):
    T, DW = res_v.shape
    H = acts.shape[0]
    TH = T // H
    TB, KC = acts.shape[-2:]
    KB = 2 * KC
    TL, NB = err.shape[-2:]
    w = lax.axis_index("width")
    l = lax.axis_index("lat")
    z, c = w // 2, w % 2
    pc = 1 - c
    partner = (z * 2 + pc, l)

    side = z // 2
    near, far_in, far_out = z + 1 - 2 * (z % 2), 2 - side, 3 - 3 * side
    inner = (z + side) % 2

    def zdev(o):
        return ((z + o) % Z) * 2 + c, l

    def on(other):
        return other * 2 + c, l

    def lat_to(o):
        return ((l // 2 + o // 2) % (NL // 2)) * 2 + (l % 2 + o % 2) % 2

    lx, ly, ld = lat_to(1), lat_to(2), lat_to(3)

    def rc(src, dst, ssem, rsem, dev):
        return pltpu.make_async_remote_copy(
            src_ref=src, dst_ref=dst, send_sem=ssem, recv_sem=rsem,
            device_id=dev, device_id_type=MESH,
        )

    def arrived(ref, sem):
        rc(ref, ref, sem, sem, partner).wait_recv()

    def left(ref, sem):
        rc(ref, ref, sem, sem, partner).wait_send()

    A1, A2, A3, A4, B1, B2, C1, C2, D1, D2, D3, D3F, D3L, D4, E1, E2 = (
        sent.at[i] for i in range(16)
    )

    def span(first, stop, f):
        lax.fori_loop(first, stop, lambda i, _: (f(i), 0)[1], 0)

    def loop(n, f):
        lax.fori_loop(0, n, lambda i, _: (f(i), 0)[1], 0)

    c_res = pltpu.make_async_copy(res_h, res_v, in_sem.at[0])
    c_res.start()

    def enc_copy(k):
        return pltpu.make_async_copy(
            enc_h.at[:, pl.ds(pl.multiple_of(k * KB, KB), KB)], enc_v.at[k], in_sem.at[1 + k]
        )

    def dec_copy(n):
        return pltpu.make_async_copy(
            dec_h.at[:, pl.ds(pl.multiple_of(n * NB, NB), NB)], dec_v.at[n], in_sem.at[1 + NK + n]
        )

    for k in range(NK):
        enc_copy(k).start()
    c_bias = pltpu.make_async_copy(bias_h, bias, in_sem.at[1 + NK + NN])
    c_dbias = pltpu.make_async_copy(dbias_h, dbias, in_sem.at[2 + NK + NN])
    c_bias.start()
    c_dbias.start()

    barrier = pltpu.get_barrier_semaphore()
    pl.semaphore_signal(barrier, inc=1, device_id=partner, device_id_type=MESH)
    for o in range(1, Z):
        pl.semaphore_signal(barrier, inc=1, device_id=zdev(o), device_id_type=MESH)
    for o in range(1, NL):
        pl.semaphore_signal(barrier, inc=1, device_id=(w, lat_to(o)), device_id_type=MESH)

    def a1(h, k):
        return rc(stA.at[h, k, pc], rxA.at[h, k], A1, r1.at[h, k], partner)

    def a2(h, k, i):
        src, dst, recv, to = (
            (sA.at[h, k, near], rA.at[h, k, 0], 0, near),
            (tA.at[h, k, 0], rA.at[h, k, 1], 0, far_in),
            (tA.at[h, k, 1], rA.at[h, k, 1], 0, far_out),
            (sA.at[h, k, far_in], qA.at[h, k, 0], 1, near),
            (sA.at[h, k, far_out], qA.at[h, k, 1], 1, near),
        )[i]
        return rc(src, dst, A2, r2.at[h, k, recv], on(to))

    def a3(h, k, o):
        block = acts.at[h, k, c, z]
        return rc(block, block, A3, r3.at[h, k, 0], zdev(o))

    def d3(h, k, o):
        block = dp.at[h, k, c, z]
        return rc(block, block, D3L, r3.at[h, k, 0], zdev(o))

    def d3_near(h, k, i):
        block, recv, to, sem = (
            (z, 0, near, D3), (z, 1, far_in, D3), (far_in, 1, near, D3F), (far_out, 1, near, D3F)
        )[i]
        block = dp.at[h, k, c, block]
        return rc(block, block, sem, r3.at[h, k, recv], on(to))

    def pass_d(h, k):
        @pl.when(inner == 1)
        def _():
            arrived(dp.at[h, k, c, 0:2], r3.at[h, k, 1])
            d3_near(h, k, 2).start()
            d3_near(h, k, 3).start()

    def own_core(ref, ssem, rsem):
        def send(h, k):
            block = ref.at[h, k, c]
            return rc(block, block, ssem, rsem.at[h, k], partner)

        def arrive(h, k):
            arrived(ref.at[h, k, pc], rsem.at[h, k])

        return send, arrive

    a4, a4in = own_core(acts, A4, r4)
    d4, d4in = own_core(dp, D4, r4)

    def combine_a(h, k):
        a1(h, k).wait_recv()
        sA[h, k] = stA[h, k, c] + rxA[h, k]

        @pl.when(inner == 0)
        def _():
            a2(h, k, 3).start()
            a2(h, k, 4).start()

        @pl.when(inner == 1)
        def _():
            a2(h, k, 0).start()

    def near_a(h, k):
        @pl.when(inner == 0)
        def _():
            a2(h, k, 0).start()

    def relay_a(h, k):
        @pl.when(inner == 1)
        def _():
            arrived(qA.at[h, k], r2.at[h, k, 1])
            for i, block in enumerate((far_in, far_out)):
                tA[h, k, i] = sA[h, k, block] + qA[h, k, i]
                a2(h, k, 1 + i).start()

    c_res.wait()
    for n in range(NN):
        dec_copy(n).start()

    def pre_part(h, k):
        p = jnp.dot(res_v[h * TH:(h + 1) * TH, :], enc_v[k], preferred_element_type=F32)
        for j in range(2):
            stA[h, k, j] = p[:, j * KC:(j + 1) * KC].reshape(Z, TB, KC)

    def pre_early(k):
        enc_copy(k).wait()
        pre_part(0, k)

    def pre_first(k):
        enc_copy(k).wait()
        pre_part(0, k)
        a1(0, k).start()
        combine_a(0, k - EARLY)

    def pre_next(h, k):
        pre_part(h, k)
        a1(h, k).start()

    EARLY = NK // 2
    loop(EARLY, pre_early)
    pl.semaphore_wait(barrier, 1 + (Z - 1) + (NL - 1))
    loop(EARLY, lambda k: a1(0, k).start())
    lax.fori_loop(EARLY, NK, lambda k, _: (pre_first(k), 0)[1], 0)
    lax.fori_loop(NK - EARLY, NK, lambda k, _: (combine_a(0, k), 0)[1], 0)
    loop(NK, lambda k: near_a(0, k))
    def second_a(h, k):
        combine_a(h, k)
        near_a(h, k)

    loop(NK, lambda k: pre_next(1, k))
    loop(NK, lambda k: second_a(1, k))
    loop(NK, lambda k: pre_next(2, k))
    c_bias.wait()
    c_dbias.wait()

    def fwd_a(h, k):
        arrived(acts.at[h, k, c, 1:Z], r3.at[h, k, 0])
        a4(h, k).start()

    def act_step(h, k):
        arrived(rA.at[h, k], r2.at[h, k, 0])
        pre = (sA[h, k, z] + rA[h, k, 0]) + rA[h, k, 1]
        pre = pre + bias[k, c]
        preS[h, k] = pre
        acts[h, k, c, z] = jnp.maximum(pre, 0.0).astype(BF16)
        for o in range(1, Z):
            a3(h, k, o).start()

    loop(NK, lambda k: relay_a(0, k))
    loop(NK, lambda k: act_step(0, k))
    loop(NK, lambda k: second_a(2, k))

    def rt_step(n):
        rt_v[n] = res_v[:, pl.ds(pl.multiple_of(n * NB, NB), NB)].T

    loop(NN, rt_step)
    loop(NK, lambda k: relay_a(1, k))

    last_n = NN - 1
    halves = (slice(0, NB // 2), slice(NB // 2, NB))

    def b1(h, n, i):
        to, block, half, dst = (
            (lx, ld, 1, fB.at[h, n, 0]),
            (ly, ld, 0, fB.at[h, n, 1]),
            (lx, lx, 1, rB.at[h, n, 0]),
            (ly, ly, 0, rB.at[h, n, 1]),
        )[i]
        return rc(sB.at[h, n, block, :, halves[half]], dst, B1, rx.at[h, n, i // 2], (w, to))

    def b2(h, n, i):
        return rc(
            tB.at[h, n, i], rB.at[h, n, 2 + i], B2, rx.at[h, n, 1], (w, (ly, lx)[i]),
        )

    def relay_b(h, n):
        arrived(fB.at[h, n], rx.at[h, n, 0])
        for i, block, half in ((0, ly, 1), (1, lx, 0)):
            tB[h, n, i] = (rf[h, n, block, :, halves[half]] + fB[h, n, i].astype(F32)).astype(BF16)
            b2(h, n, i).start()

    def c1(h, n, i):
        block = err.at[h, n, l]
        return rc(block, block, C1, rx.at[h, n, 0], (w, (lx, ly)[i]))

    def c2(h, n, i):
        block = err.at[h, n, (lx, ly)[i], :, halves[1 - i]]
        return rc(block, block, C2, rx.at[h, n, 1], (w, (ly, lx)[i]))

    def fwd_c(h, n):
        arrived(err.at[h, n, 0:2], rx.at[h, n, 0])
        for i in range(2):
            c2(h, n, i).start()

    def rec_step(h, n):
        a = jnp.concatenate(
            [acts[h, k, j].reshape(TH, KC) for k in range(NK) for j in range(2)], axis=1
        )
        r = jnp.dot(a, dec_v[n], preferred_element_type=F32).reshape(NL, TL, NB)
        rf[h, n] = r
        sB[h, n] = r.astype(BF16)
        for i in range(4):
            b1(h, n, i).start()

    def at_step(h, k):
        a = jnp.concatenate([acts[h, k, j].reshape(TH, KC) for j in range(2)], axis=1)
        actsT[k, :, h * TH:(h + 1) * TH] = a.T

    def err_step(h, n):
        arrived(rB.at[h, n], rx.at[h, n, 1])
        for half in range(2):
            cols = halves[half]
            r = rf[h, n, l, :, cols]
            for j in (1 - half, 3 - half):
                r = r + rB[h, n, j].astype(F32)
            own = res_v[
                pl.ds(pl.multiple_of(h * TH + l * TL, TL), TL),
                pl.ds(pl.multiple_of(n * NB + half * (NB // 2), NB // 2), NB // 2),
            ]
            err[h, n, l, :, cols] = (r + dbias[n, :, cols] - own.astype(F32)).astype(BF16)
        for i in range(2):
            c1(h, n, i).start()

    loop(NK, lambda k: fwd_a(0, k))
    for n in range(NN):
        dec_copy(n).wait()
    loop(NK, lambda k: a4in(0, k))
    loop(NN, lambda n: rec_step(0, n))
    loop(NK, lambda k: act_step(1, k))
    loop(NK, lambda k: relay_a(2, k))
    loop(NK, lambda k: at_step(0, k))

    def zero_step(k):
        for s in range(1, 3):
            sacc[s, k] = jnp.zeros(sacc.shape[2:], F32)

    loop(NK, zero_step)

    loop(NN, lambda n: relay_b(0, n))
    span(0, NN // 2, lambda n: err_step(0, n))
    loop(NK, lambda k: fwd_a(1, k))
    span(NN // 2, last_n, lambda n: err_step(0, n))
    loop(NK, lambda k: a4in(1, k))
    span(0, NN // 2, lambda n: rec_step(1, n))
    err_step(0, last_n)
    span(NN // 2, NN, lambda n: rec_step(1, n))
    loop(NK, lambda k: act_step(2, k))
    span(0, last_n, lambda n: fwd_c(0, n))
    span(0, NN // 2, lambda n: relay_b(1, n))
    fwd_c(0, last_n)
    loop(NK, lambda k: at_step(1, k))
    span(NN // 2, NN, lambda n: relay_b(1, n))

    def dec_rows(n, k):
        return dec_v[n, pl.ds(pl.multiple_of(k * KB, KB), KB), :]

    def dacts_part(h, n, k):
        d = lax.dot_general(
            err[h, n].reshape(TH, NB), dec_rows(n, k), NT, preferred_element_type=F32
        )
        return [d[:, j * KC:(j + 1) * KC].reshape(Z, TB, KC) for j in range(2)]

    def grad_first(n, k):
        grad[n, k] = jnp.dot(
            actsT[k, :, 0:2 * TH], err[0:2, n].reshape(2 * TH, NB), preferred_element_type=F32
        )

    def grad_last(n, k):
        g = grad[n, k] + jnp.dot(
            actsT[k, :, 2 * TH:T], err[2, n].reshape(TH, NB), preferred_element_type=F32
        )
        grad[n, k] = g
        wt = dec_rows(n, k).astype(F32)
        for s, prod in ((1, g * wt), (2, g * g)):
            part = prod[:, 0:128]
            for j in range(1, NB // 128):
                part = part + prod[:, j * 128:(j + 1) * 128]
            sacc[s, k] += part

    def err_wait(h, n):
        arrived(err.at[h, n, 0], rx.at[h, n, 1])

    def d1(h, k):
        return rc(sD.at[h, k, pc], rxD.at[h, k], D1, r1.at[h, k], partner)

    def d2(h, k, o):
        return rc(
            sS.at[h, k, (z + o) % Z], rD.at[h, k, o], D2, r2.at[h, k, 0], zdev(o)
        )

    def combine_d(h, k):
        d1(h, k).wait_recv()
        s = dacc[h, k, c] + rxD[h, k].astype(F32)
        dacc[h, k, c] = s
        sS[h, k] = s.astype(BF16)
        for o in range(1, Z):
            d2(h, k, o).start()

    def dacts_add(h, n, k):
        for j, d in enumerate(dacts_part(h, n, k)):
            if isinstance(n, int) and n == 0:
                dacc[h, k, j] = d
            else:
                dacc[h, k, j] += d

    last = NN - 1

    def d_step(h, k):
        for j, d in enumerate(dacts_part(h, last, k)):
            v = dacc[h, k, j] + d
            dacc[h, k, j] = v
            sD[h, k, j] = v.astype(BF16)
        d1(h, k).start()

    def dacts(h, n):
        err_wait(h, n)
        for k in range(NK):
            dacts_add(h, n, k)

    def d_steps(h):
        err_wait(h, last)
        for k in range(NK):
            d_step(h, k)

    def dp_step(h, k):
        arrived(rD.at[h, k, 1:Z], r2.at[h, k, 0])
        v = dacc[h, k, c, z]
        for o in range(1, Z):
            v = v + rD[h, k, o].astype(F32)
        dp[h, k, c, z] = jnp.where(preS[h, k] > 0.0, v + PENALTY, 0.0).astype(BF16)
        if h < 2:
            d3_near(h, k, 0).start()
            d3_near(h, k, 1).start()
        else:
            for o in range(1, Z):
                d3(h, k, o).start()

    def fwd_d(h, k):
        if h < 2:
            @pl.when(inner == 0)
            def _():
                arrived(dp.at[h, k, c, 0:2], r3.at[h, k, 1])

            arrived(dp.at[h, k, c, 0], r3.at[h, k, 0])
        else:
            arrived(dp.at[h, k, c, 1:Z], r3.at[h, k, 0])
        d4(h, k).start()

    def grad_n(n):
        for k in range(NK):
            grad_first(n, k)

    def ww_step(k):
        total = jnp.zeros(sacc.shape[2:], F32)
        for n in range(NN):
            wt = dec_rows(n, k).astype(F32)
            prod = wt * wt
            for j in range(NB // 128):
                total = total + prod[:, j * 128:(j + 1) * 128]
        sacc[0, k] = total

    def err_dacts(n):
        err_step(2, n)
        dacts(1, n)

    loop(NK, lambda k: fwd_a(2, k))
    err_step(1, 0)
    dacts(0, 0)
    err_step(1, 1)
    loop(NK, lambda k: a4in(2, k))

    def err_rec(n):
        rec_step(2, n - NN // 2)
        err_step(1, n)

    span(NN // 2, NN, err_rec)
    span(NN - NN // 2, NN, lambda n: rec_step(2, n))

    def dacts_fwd(n):
        dacts(0, n)
        fwd_c(1, n - 1)

    span(1, last, dacts_fwd)
    relay_b(2, 0)
    d_steps(0)
    fwd_c(1, NN - 2)
    span(1, NN - 2, lambda n: relay_b(2, n))
    fwd_c(1, NN - 1)
    loop(NK, lambda k: combine_d(0, k))
    relay_b(2, NN - 2)
    loop(NK, lambda k: at_step(2, k))
    relay_b(2, NN - 1)
    loop(NK, ww_step)
    err_dacts(0)
    span(1, last, err_dacts)
    err_step(2, last)
    d_steps(1)
    fwd_c(2, 0)
    loop(NK, lambda k: combine_d(1, k))
    loop(NK, lambda k: dp_step(0, k))
    fwd_c(2, 1)
    grad_n(0)
    fwd_c(2, 2)
    grad_n(1)
    fwd_c(2, 3)
    grad_n(2)
    grad_n(3)
    dacts(2, 0)
    span(1, last, lambda n: dacts(2, n))
    d_steps(2)
    loop(NK, lambda k: combine_d(2, k))
    loop(NK, lambda k: dp_step(1, k))
    loop(NK, lambda k: pass_d(0, k))

    def grads_last(n):
        for k in range(NK):
            grad_last(n, k)

    span(0, last, grads_last)

    def st_row(s, k, j):
        return (k * 3 + s) * (KB // 128) + j

    def gd_step(k):
        grad_last(last, k)
        for s in range(3):
            total = jnp.sum(sacc[s, k].T, axis=0, keepdims=True)
            for j in range(KB // 128):
                stv[pl.ds(st_row(s, k, j), 1), :] = total[:, j * 128:(j + 1) * 128]

    for k in range(NK):
        gd_step(k)

    e1 = rc(stv, rst, E1, e1r, partner)
    e1.start()

    def e2(o):
        return rc(ss, rs2.at[o], E2, e2r, zdev(o))

    e1.wait_recv()
    ss[...] = stv[...] + rst[...]
    for o in range(1, Z):
        e2(o).start()
    loop(NK, lambda k: dp_step(2, k))
    loop(NK, lambda k: pass_d(1, k))
    loop(NK, lambda k: fwd_d(0, k))
    arrived(rs2.at[1:Z], e2r)

    total = ss[...]
    for o in range(1, Z):
        total = total + rs2[o]
    st[...] = total

    def nd_step(k):
        ww, gw, gg = (
            jnp.concatenate(
                [st[pl.ds(st_row(s, k, j), 1), :] for j in range(KB // 128)], axis=1
            )
            for s in range(3)
        )
        coef = gw / (ww + EPS)
        sq = (
            ww
            - 2.0 * STEP * (gw - coef * ww)
            + STEP * STEP * (gg - 2.0 * coef * gw + coef * coef * ww)
        )
        inv = 1.0 / jnp.sqrt(sq + EPS)
        up = jnp.broadcast_to((1.0 + STEP * coef) * inv, (128, KB)).T
        down = jnp.broadcast_to(STEP * inv, (128, KB)).T
        for n in range(NN):
            for j in range(NB // 128):
                wt = dec_v[n, pl.ds(pl.multiple_of(k * KB, KB), KB), j * 128:(j + 1) * 128]
                g = grad[n, k, :, j * 128:(j + 1) * 128]
                first = n * NB + j * 128
                nd_v[k, :, first:first + 128] = (wt.astype(F32) * up - g * down).astype(BF16)

    loop(NK, nd_step)
    loop(NK, lambda k: fwd_d(1, k))
    loop(NK, lambda k: fwd_d(2, k))
    for h in range(H):
        loop(NK, lambda k: d4in(h, k))

    for ref, sem in (
        (rxA, A1), (sA.at[:, :, 1:Z], A2), (acts.at[:, :, 0, 1:Z], A3),
        (acts.at[:, :, 0], A4), (rB, B1), (tB, B2), (err.at[:, :, 0:2], C1), (err.at[:, :, 0], C2),
        (sD.at[:, :, 0], D1), (sS.at[:, :, 1:Z], D2), (dp.at[0:2, :, 0, 0:2], D3), (dp.at[2, :, 0, 1:Z], D3L),
        (dp.at[:, :, 0], D4), (ss, E1), (rs2.at[1:Z], E2),
    ):
        left(ref, sem)

    @pl.when(inner == 1)
    def _():
        left(dp.at[0:2, :, 0, 0:2], D3F)

def finish_kernel(rt, dp, nd, eg_o, nd_o, eg_v, sem):
    halves, blocks = dp.shape[:2]
    NN, NB = rt.shape[:2]
    NK, KB = nd.shape[:2]
    copies = [
        pltpu.make_async_copy(nd.at[k], nd_o.at[k * KB:(k + 1) * KB, :], sem.at[k])
        for k in range(NK)
    ]
    for copy in copies:
        copy.start()
    d = jnp.concatenate(
        [
            jnp.concatenate([dp[h, k] for k in range(blocks)], axis=1)
            for h in range(halves)
        ],
        axis=0,
    )
    for n in range(NN):
        eg_v[n] = jnp.dot(rt[n], d, preferred_element_type=F32).astype(BF16)
        copy = pltpu.make_async_copy(eg_v.at[n], eg_o.at[n * NB:(n + 1) * NB, :], sem.at[NK + n])
        copy.start()
        copies.append(copy)
    for copy in copies:
        copy.wait()


def fused(W, NL, residuals, encoder, enc_bias, decoder, dec_bias):
    T, DW = residuals.shape
    LL = encoder.shape[1]
    Z = W // 2
    NK, NN = 4, 4
    KB, NB = LL // NK, DW // NN
    H = 3
    TH = T // H
    TB, TL = TH // Z, TH // NL
    KC = KB // 2
    V = pltpu.VMEM
    dma = pltpu.SemaphoreType.DMA
    sums, part, rows = (H, NK, 2, Z, TB, KC), (H, NK, Z, TB, KC), (H, NN, NL, TL, NB)
    stats = (3 * LL // 128, 128)
    one, two = (H, NK), (H, NK, 2)
    half, pair = (TL, NB // 2), (H, NK, 2, TB, KC)
    scratch = [
        V((T, DW), BF16), V((NK, DW, KB), BF16), V((NN, LL, NB), BF16),
        V((NK, 2, 1, KC), F32), V((NN, 1, NB), F32),
        V(sums, F32), V(part, F32), V(part, F32), V(pair, F32), V(pair, F32), V(pair, F32),
        V((H, NK, TB, KC), F32),
        V(sums, BF16), V((NK, KB, T), BF16),
        V(rows, F32), V(rows, BF16), V((H, NN, 2, *half), BF16), V((H, NN, 2, *half), BF16),
        V((H, NN, 4, *half), BF16), V(rows, BF16),
        V(sums, F32), V(sums, BF16), V(part, BF16), V(part, BF16), V(part, BF16),
        V((NN, NK, KB, NB), F32), V((3, NK, KB, 128), F32),
        V(stats, F32), V(stats, F32), V(stats, F32), V((Z, *stats), F32), V(stats, F32),
        dma((3 + NK + NN,)), dma((16,)),
        dma(one), dma(two), dma(two), dma(one), dma((H, NN, 2)), dma, dma,
    ]
    hbm = pl.BlockSpec(memory_space=pltpu.HBM)
    vm = pl.BlockSpec(memory_space=pltpu.VMEM)
    new_decoder, dp, rt = pl.pallas_call(
        functools.partial(step_kernel, Z, NL, NK, NN),
        out_shape=(
            V((NK, KB, DW), BF16),
            V(sums, BF16),
            V((NN, NB, T), BF16),
        ),
        in_specs=[hbm] * 5,
        out_specs=(vm, vm, vm),
        scratch_shapes=scratch,
        compiler_params=pltpu.CompilerParams(
            collective_id=0, has_side_effects=True, vmem_limit_bytes=115 * 2**19
        ),
        name="sae_step",
    )(residuals, encoder, enc_bias.reshape(NK, 2, 1, KC), decoder, dec_bias.reshape(NN, 1, NB))
    return pl.pallas_call(
        finish_kernel,
        out_shape=(
            jax.ShapeDtypeStruct((DW, LL), BF16),
            jax.ShapeDtypeStruct((LL, DW), BF16),
        ),
        in_specs=[vm, vm, vm],
        out_specs=(hbm, hbm),
        scratch_shapes=[V((NN, NB, LL), BF16), dma((NK + NN,))],
        compiler_params=pltpu.CompilerParams(vmem_limit_bytes=30 * 2**20),
        cost_estimate=pl.CostEstimate(
            flops=2 * T * DW * LL, bytes_accessed=4 * DW * LL, transcendentals=0,
        ),
        name="finish",
    )(rt, dp.reshape(H, 2 * NK, TH, KC), new_decoder)


def plain(residuals, encoder, enc_bias, decoder, dec_bias):
    tokens = residuals.shape[0]
    lat_count = lax.axis_size("lat")
    lat_rows = tokens // lat_count
    rows = residuals
    pre_rows = (
        lax.psum_scatter(
            jnp.dot(rows, encoder, preferred_element_type=jnp.float32),
            "width",
            scatter_dimension=0,
            tiled=True,
        )
        + enc_bias
    )
    active_rows = pre_rows > 0.0
    act_rows = jnp.maximum(pre_rows, 0.0).astype(jnp.bfloat16)
    acts = lax.all_gather(act_rows, "width", axis=0, tiled=True)
    rows = acts
    recon_rows = lax.psum_scatter(
        jnp.dot(rows, decoder, preferred_element_type=jnp.float32),
        "lat",
        scatter_dimension=0,
        tiled=True,
    )
    first = lax.axis_index("lat") * lat_rows
    own_rows = lax.dynamic_slice_in_dim(residuals, first, lat_rows, 0)
    error_part = (recon_rows + dec_bias - own_rows.astype(jnp.float32)).astype(jnp.bfloat16)
    error = lax.all_gather(error_part, "lat", axis=0, tiled=True)
    rows = error
    dacts_rows = (
        lax.psum_scatter(
            lax.dot_general(
                rows, decoder, (((1,), (1,)), ((), ())), preferred_element_type=jnp.float32
            ),
            "width",
            scatter_dimension=0,
            tiled=True,
        )
        + PENALTY
    )
    dpre_part = jnp.where(active_rows, dacts_rows, 0.0).astype(jnp.bfloat16)
    dpre = lax.all_gather(dpre_part, "width", axis=0, tiled=True)
    enc_grad = lax.dot_general(
        residuals, dpre, (((0,), (0,)), ((), ())), preferred_element_type=jnp.float32
    ).astype(jnp.bfloat16)
    grad = lax.dot_general(
        acts, error, (((0,), (0,)), ((), ())), preferred_element_type=jnp.float32
    )
    weight = decoder.astype(jnp.float32)
    ww, gw, gg = lax.psum(
        (
            jnp.sum(weight * weight, axis=1),
            jnp.sum(grad * weight, axis=1),
            jnp.sum(grad * grad, axis=1),
        ),
        "width",
    )
    coef_row = gw / (ww + EPS)
    coef = coef_row[:, None]
    moved = weight - STEP * (grad - coef * weight)
    squared = (
        ww
        - 2.0 * STEP * (gw - coef_row * ww)
        + STEP * STEP * (gg - 2.0 * coef_row * gw + coef_row * coef_row * ww)
    )
    new_decoder = (moved / jnp.sqrt(squared + EPS)[:, None]).astype(jnp.bfloat16)
    return (enc_grad, new_decoder)


def per_device(W, NL, residuals, encoder, enc_bias, decoder, dec_bias):
    T, DW = residuals.shape
    LL = encoder.shape[1]
    args = (residuals, encoder, enc_bias, decoder, dec_bias)
    fits = W == 8 and NL == 4 and T % (48 * NL) == 0
    if fits and DW % 512 == 0 and LL % 1024 == 0 and T % 128 == 0:
        return fused(W, NL, *args)
    return plain(*args)


def solution(mesh):
    return jax.shard_map(
        functools.partial(per_device, mesh.shape["width"], mesh.shape["lat"]),
        mesh=mesh,
        in_specs=(P(None, "width"), P("width", "lat"), P("lat"), P("lat", "width"), P("width")),
        out_specs=(P("width", "lat"), P("lat", "width")),
        check_vma=False,
    )
```
